16 devices in a mesh: data: 16 (over z, y, x, core).
Axes of the slice: x: 2, y: 2, z: 2, core: 2. Of those that a mesh axis runs over, the one named last changes fastest.
Arguments:
- x_tokens: bfloat16 [65536, 1024], P('data')
- dh_out: bfloat16 [65536, 1024], P('data')
- w_up: bfloat16 [2, 1024, 2736], replicated
- w_down: bfloat16 [2, 2736, 1024], replicated
- proj_up: bfloat16 [2, 1024, 256], replicated
- proj_down: bfloat16 [2, 1024, 256], replicated
- mom_up: float32 [2, 256, 2736], P(None, None, 'data')
- var_up: float32 [2, 256, 2736], P(None, None, 'data')
- mom_down: float32 [2, 2736, 256], P(None, 'data')
- var_down: float32 [2, 2736, 256], P(None, 'data')
Outputs:
- output 1: bfloat16 [2, 1024, 2736], replicated
- output 2: bfloat16 [2, 2736, 1024], replicated
- output 3: float32 [2, 256, 2736], P(None, None, 'data')
- output 4: float32 [2, 256, 2736], P(None, None, 'data')
- output 5: float32 [2, 2736, 256], P(None, 'data')
- output 6: float32 [2, 2736, 256], P(None, 'data')
All inputs are finite; a program needn't handle non-finite values.
Results may differ from the reference program's by a relative error of at most 0.00726549.
Values are sent between devices in bfloat16 or wider.
A program may use at most 1 GiB of HBM per device.

```python
import jax
import jax.numpy as jnp
from jax import lax

D = 1024
FF = 2736
RANK = 256
TOKENS = 65536
BLOCK = 2048
STEP = 4
BETA_ONE = 0.9
BETA_TWO = 0.999
EPSILON = 1e-8
LEARN_RATE = 0.02
ALPHA_SCALE = 0.25


def setup_inputs(seed: int = 0) -> dict:
    key_list = jax.random.split(jax.random.key(seed), 10)
    x_tokens = jax.random.normal(key_list[0], (TOKENS, D), jnp.float32)
    dh_out = jax.random.normal(key_list[1], (TOKENS, D), jnp.float32) * (20.0 * TOKENS ** -0.5)
    w_up = jax.random.normal(key_list[2], (2, D, FF), jnp.float32) * D ** -0.5
    w_down = jax.random.normal(key_list[3], (2, FF, D), jnp.float32) * FF ** -0.5
    proj_up = jnp.linalg.qr(jax.random.normal(key_list[4], (2, D, RANK), jnp.float32))[0]
    proj_down = jnp.linalg.qr(jax.random.normal(key_list[5], (2, D, RANK), jnp.float32))[0]
    mom_up = jax.random.normal(key_list[6], (2, RANK, FF), jnp.float32)
    var_up = jax.random.uniform(key_list[7], (2, RANK, FF), jnp.float32, 0.05, 0.15)
    mom_down = jax.random.normal(key_list[8], (2, FF, RANK), jnp.float32)
    var_down = jax.random.uniform(key_list[9], (2, FF, RANK), jnp.float32, 0.05, 0.15)
    return {
        'x_tokens': x_tokens.astype(jnp.bfloat16),
        'dh_out': dh_out.astype(jnp.bfloat16),
        'w_up': w_up.astype(jnp.bfloat16),
        'w_down': w_down.astype(jnp.bfloat16),
        'proj_up': proj_up.astype(jnp.bfloat16),
        'proj_down': proj_down.astype(jnp.bfloat16),
        'mom_up': mom_up,
        'var_up': var_up,
        'mom_down': mom_down,
        'var_down': var_down,
    }


def block_grads(x_rows, dh_rows, w_up, w_down, proj_up, proj_down):
    hidden = [x_rows]
    act_list = []
    pull_list = []
    for layer_idx in range(2):
        pre_act = jnp.dot(hidden[layer_idx], w_up[layer_idx], preferred_element_type=jnp.float32)
        gelu_val, gelu_pull = jax.vjp(jax.nn.gelu, pre_act)
        act_val = gelu_val.astype(jnp.bfloat16)
        down_out = jnp.dot(act_val, w_down[layer_idx], preferred_element_type=jnp.float32)
        hidden.append((hidden[layer_idx].astype(jnp.float32) + down_out).astype(jnp.bfloat16))
        act_list.append(act_val)
        pull_list.append(gelu_pull)
    grad_rows = dh_rows
    up_parts = [None, None]
    down_parts = [None, None]
    for layer_idx in (1, 0):
        v_proj = jnp.dot(grad_rows, proj_down[layer_idx], preferred_element_type=jnp.float32).astype(jnp.bfloat16)
        down_parts[layer_idx] = jnp.dot(act_list[layer_idx].T, v_proj, preferred_element_type=jnp.float32)
        d_act = jnp.dot(grad_rows, w_down[layer_idx].T, preferred_element_type=jnp.float32)
        d_pre = pull_list[layer_idx](d_act)[0].astype(jnp.bfloat16)
        u_proj = jnp.dot(hidden[layer_idx], proj_up[layer_idx], preferred_element_type=jnp.float32).astype(jnp.bfloat16)
        up_parts[layer_idx] = jnp.dot(u_proj.T, d_pre, preferred_element_type=jnp.float32)
        if layer_idx > 0:
            back_term = jnp.dot(d_pre, w_up[layer_idx].T, preferred_element_type=jnp.float32)
            grad_rows = (grad_rows.astype(jnp.float32) + back_term).astype(jnp.bfloat16)
    return jnp.stack(up_parts), jnp.stack(down_parts)


def adam_step(moment, variance, grad_red):
    new_mom = BETA_ONE * moment + (1.0 - BETA_ONE) * grad_red
    new_var = BETA_TWO * variance + (1.0 - BETA_TWO) * grad_red * grad_red
    bias_one = 1.0 - BETA_ONE ** STEP
    bias_two = 1.0 - BETA_TWO ** STEP
    direction = (new_mom / bias_one) / (jnp.sqrt(new_var / bias_two) + EPSILON)
    return new_mom, new_var, direction.astype(jnp.bfloat16)


def reference(x_tokens, dh_out, w_up, w_down, proj_up, proj_down, mom_up, var_up, mom_down, var_down):
    x_blocks = x_tokens.reshape(TOKENS // BLOCK, BLOCK, D)
    dh_blocks = dh_out.reshape(TOKENS // BLOCK, BLOCK, D)

    def scan_body(carry_acc, block_pair):
        part_up, part_down = block_grads(block_pair[0], block_pair[1], w_up, w_down, proj_up, proj_down)
        return (carry_acc[0] + part_up, carry_acc[1] + part_down), None

    zero_init = (jnp.zeros((2, RANK, FF), jnp.float32), jnp.zeros((2, FF, RANK), jnp.float32))
    scan_out = lax.scan(scan_body, zero_init, (x_blocks, dh_blocks))
    red_up, red_down = scan_out[0]
    new_mom_up, new_var_up, dir_up = adam_step(mom_up, var_up, red_up)
    new_mom_down, new_var_down, dir_down = adam_step(mom_down, var_down, red_down)
    delta_up = jnp.einsum('ldr,lrf->ldf', proj_up.astype(jnp.float32), dir_up.astype(jnp.float32))
    delta_down = jnp.einsum('lfr,ldr->lfd', dir_down.astype(jnp.float32), proj_down.astype(jnp.float32))
    new_w_up = (w_up.astype(jnp.float32) - (LEARN_RATE * ALPHA_SCALE) * delta_up).astype(jnp.bfloat16)
    new_w_down = (w_down.astype(jnp.float32) - (LEARN_RATE * ALPHA_SCALE) * delta_down).astype(jnp.bfloat16)
    return (new_w_up, new_w_down, new_mom_up, new_var_up, new_mom_down, new_var_down)
```

```python
import functools

import jax
import jax.numpy as jnp
from jax import lax
from jax.experimental import pallas as pl
from jax.experimental.pallas import tpu as pltpu
from jax.sharding import PartitionSpec as P

BETA_ONE = 0.9
BETA_TWO = 0.999
EPSILON = 1e-8
STEP = 4
LEARN_RATE = 0.02
ALPHA_SCALE = 0.25

C0 = 0.7978845608028654
C1 = C0 * 0.044715
D = 1024
FF = 2736
RANK = 256
DEV = 16
SHARD = FF // DEV
PAD = 176
FFP = DEV * PAD
F32 = jnp.float32
BF16 = jnp.bfloat16


def spans_of(width):
    return [(s, min(width, FF - s)) for s in range(0, FF, width)]


def dot_nn(a, b):
    return lax.dot_general(a, b, (((1,), (0,)), ((), ())), preferred_element_type=F32)


def dot_nt(a, b):
    return lax.dot_general(a, b, (((1,), (1,)), ((), ())), preferred_element_type=F32)


def gelu_val(z):
    z2 = z * z
    t = jnp.tanh(z * (C0 + C1 * z2))
    return z * (0.5 * t + 0.5)


def gelu_both(z):
    z2 = z * z
    t = jnp.tanh(z * (C0 + C1 * z2))
    c = 0.5 * t + 0.5
    a = z * c
    slope = c + (a - a * c) * (2.0 * C0 + 6.0 * C1 * z2)
    return a, slope


ANY = pl.BlockSpec(memory_space=pl.ANY)
ONCE = pl.Buffered(1)


def kernel_a(tile, tiles, x_ref, dh_ref, p_ref, q_ref, w1_hbm, w2_hbm,
             z0_hbm, g1_ref, u0_ref, r_hbm,
             w1a, w2a, w1b, w2b, z0, a0, h1, dz1, zs, das, ac, u1, v1, r1, r2, r3, rt, blk, sem, zsem):
    i = pl.program_id(0)
    width, slab = 512, 16
    spans = spans_of(width)
    loads = [
        pltpu.make_async_copy(w1_hbm.at[0], w1a, sem.at[0]),
        pltpu.make_async_copy(w2_hbm.at[0], w2a, sem.at[1]),
        pltpu.make_async_copy(w1_hbm.at[1], w1b, sem.at[2]),
        pltpu.make_async_copy(w2_hbm.at[1], w2b, sem.at[3]),
    ]

    def z_out(idx):
        return pltpu.make_async_copy(z0, z0_hbm.at[pl.ds(pl.multiple_of(idx * tile, tile), tile)], zsem)

    @pl.when(i == 0)
    def _():
        for cp in loads:
            cp.start()
        r1[...] = jnp.zeros_like(r1)
        r2[...] = jnp.zeros_like(r2)
        r3[...] = jnp.zeros_like(r3)

    x = x_ref[...]
    u0_ref[...] = dot_nn(x, p_ref[0]).T.astype(BF16)
    v1[...] = dot_nn(dh_ref[...], q_ref[1]).T.astype(BF16)

    @pl.when(i == 0)
    def _():
        loads[0].wait()

    @pl.when(i > 0)
    def _():
        z_out(i - 1).wait()

    def act0(span):
        s, w = span
        for r in range(0, tile, slab):
            a0[r:r + slab, s:s + w] = gelu_val(z0[r:r + slab, s:s + w]).astype(BF16)

    prev = None
    for span in spans:
        s, w = span
        z0[:, s:s + w] = dot_nt(x, w1a[s:s + w, :])
        if prev is not None:
            act0(prev)
        prev = span
    act0(prev)
    z_out(i).start()

    @pl.when(i == 0)
    def _():
        for cp in loads[1:]:
            cp.wait()

    for n in range(0, D, width):
        h1[:, n:n + width] = (x_ref[:, n:n + width].astype(F32) + dot_nn(a0[...], w2a[:, n:n + width])).astype(BF16)

    u1[...] = dot_nn(h1[...], p_ref[1]).T.astype(BF16)

    def act1(span, k):
        s, w = span
        for r in range(0, tile, slab):
            a, g = gelu_both(zs[k, r:r + slab, :w])
            ac[k, r:r + slab, :w] = a.astype(BF16)
            dz1[r:r + slab, s:s + w] = (g * das[k, r:r + slab, :w]).astype(BF16)

    def acc1(span, k):
        s, w = span
        r2[:, s:s + w] += dot_nn(v1[...], ac[k, :, :w])
        r1[:, s:s + w] += dot_nn(u1[...], dz1[:, s:s + w])

    h = h1[...]
    dh = dh_ref[...]
    spans = spans_of(256)
    n = len(spans)
    for j in range(n + 2):
        if j < n:
            s, w = spans[j]
            zs[j % 2, :, :w] = dot_nt(h, w1b[s:s + w, :])
            das[j % 2, :, :w] = dot_nt(dh, w2b[s:s + w, :])
        if 1 <= j <= n:
            act1(spans[j - 1], (j - 1) % 2)
        if j >= 2:
            acc1(spans[j - 2], (j - 2) % 2)

    for n in range(0, D, width):
        g1_ref[:, n:n + width] = (dh_ref[:, n:n + width].astype(F32) + dot_nn(dz1[...], w1b[:, n:n + width])).astype(BF16)
    v0 = dot_nn(g1_ref[...], q_ref[0]).T.astype(BF16)
    for s, w in spans:
        r3[:, s:s + w] += dot_nn(v0, a0[:, s:s + w])

    @pl.when(i == tiles - 1)
    def _():
        z_out(i).wait()
        for k, acc in enumerate((r1, r2, r3)):
            for s in range(0, FFP, 256):
                rt[s:s + 256, :] = acc[:, s:s + 256].T
            if k > 0:
                pltpu.make_async_copy(blk, r_hbm.at[:, (k - 1) * PAD:k * PAD, :], sem.at[k - 1]).wait()
            for d in range(DEV):
                blk[(d % 2) * 8 + d // 2] = rt[SHARD * d:SHARD * d + PAD, :]
            pltpu.make_async_copy(blk, r_hbm.at[:, k * PAD:(k + 1) * PAD, :], sem.at[k]).start()
        pltpu.make_async_copy(blk, r_hbm.at[:, 2 * PAD:, :], sem.at[2]).wait()


def call_a(x, dh, p, q, w1, w2):
    rows, tile = x.shape[0], 512
    tiles = rows // tile
    whole = pl.BlockSpec((2, D, RANK), lambda i: (0, 0, 0), pipeline_mode=ONCE)
    rowspec = pl.BlockSpec((tile, D), lambda i: (i, 0))
    colspec = pl.BlockSpec((RANK, tile), lambda i: (0, i))
    return pl.pallas_call(
        functools.partial(kernel_a, tile, tiles),
        grid=(tiles,),
        in_specs=[rowspec, rowspec, whole, whole, ANY, ANY],
        out_specs=[ANY, rowspec, colspec, ANY],
        out_shape=[
            jax.ShapeDtypeStruct((rows, FF), F32),
            jax.ShapeDtypeStruct((rows, D), BF16),
            jax.ShapeDtypeStruct((RANK, rows), BF16),
            jax.ShapeDtypeStruct((DEV, 3 * PAD, RANK), F32),
        ],
        scratch_shapes=[
            pltpu.VMEM((FF, D), BF16), pltpu.VMEM((FF, D), BF16),
            pltpu.VMEM((FF, D), BF16), pltpu.VMEM((FF, D), BF16),
            pltpu.VMEM((tile, FF), F32), pltpu.VMEM((tile, FF), BF16),
            pltpu.VMEM((tile, D), BF16), pltpu.VMEM((tile, FF), BF16),
            pltpu.VMEM((2, tile, 256), F32), pltpu.VMEM((2, tile, 256), F32), pltpu.VMEM((2, tile, 256), BF16),
            pltpu.VMEM((RANK, tile), BF16), pltpu.VMEM((RANK, tile), BF16),
            pltpu.VMEM((RANK, FFP), F32), pltpu.VMEM((RANK, FFP), F32), pltpu.VMEM((RANK, FFP), F32),
            pltpu.VMEM((FFP, RANK), F32), pltpu.VMEM((DEV, PAD, RANK), F32),
            pltpu.SemaphoreType.DMA((4,)), pltpu.SemaphoreType.DMA,
        ],
        compiler_params=pltpu.CompilerParams(
            dimension_semantics=("arbitrary",), vmem_limit_bytes=67000000),
        cost_estimate=pl.CostEstimate(flops=140 * 10**9, bytes_accessed=110 * 10**6, transcendentals=0),
        name="pass_a",
    )(x, dh, p, q, w1, w2)


def adam_shard(moment, variance, grad_red):
    new_mom = BETA_ONE * moment + (1.0 - BETA_ONE) * grad_red
    new_var = BETA_TWO * variance + (1.0 - BETA_TWO) * grad_red * grad_red
    bias_one = 1.0 - BETA_ONE ** STEP
    bias_two = 1.0 - BETA_TWO ** STEP
    direction = (new_mom / bias_one) / (jnp.sqrt(new_var / bias_two) + EPSILON)
    return new_mom, new_var, direction


AXES = ((2, 1, 0), (1, 0, 2), (0, 2, 1))
RS_Y = ((0, 56), (56, 56), (112, 64))
AG_Y = ((0, 48), (48, 64), (112, 64))
KIND_X = (1, 3, 2)
MESH = pl.DeviceIdType.MESH


def view(fixed, rows):
    return tuple(fixed.get(a, slice(None)) for a in range(3)) + (pl.ds(*rows), slice(None))


def kernel_d(tile, tiles, width, chunks,
             z0_ref, w2_ref, mu, vu, md, vd, g1_hbm, u0_hbm, rx_hbm,
             mu_o, vu_o, md_o, vd_o, n_hbm,
             g1, u0, das, dz, acc_s, racc, rt,
             own_x, x0, x1, x2, x3, own_y, y0, y1, y2, y3, gat, tmp, nb,
             lsem, rx_s, rx_r, ry_s, ry_r, ag_s, ag_r, nsem):
    j = pl.program_id(0)
    slab = 16
    me = lax.axis_index('data')
    bits = [lax.rem(me // (8 >> a), 2) for a in range(4)]
    peer = [me + (1 - 2 * bits[a]) * (8 >> a) for a in range(4)]
    core = bits[3]
    home = {a: bits[a] for a in range(3)}

    def remote(src, dst, s, r, axis):
        return pltpu.make_async_remote_copy(src_ref=src, dst_ref=dst, send_sem=s, recv_sem=r,
                                            device_id=(peer[axis],), device_id_type=MESH)

    def flow_x(h, p):
        return (lambda spot: own_x.at[spot], lambda spot: rx_hbm.at[(1 - core,) + spot], (x0, x1, x2, x3),
                (p * PAD + h * 88, 88), AXES[p], lambda st: (rx_s.at[h, p, st], rx_r.at[h, p, st]))

    def flow_y(p):
        return (lambda spot: own_y.at[(core,) + spot], lambda spot: own_y.at[(1 - core,) + spot], (y0, y1, y2, y3),
                RS_Y[p], AXES[p], lambda st: (ry_s.at[p, st], ry_r.at[p, st]))

    def rs_copy(flow, stage):
        own, away_src, bufs, rows, axes, sems = flow
        s, r = sems(stage)
        if stage == 0:
            spot = view({}, rows)
            return remote(away_src(spot), bufs[0].at[spot], s, r, 3)
        axis = axes[stage - 1]
        away = {a: bits[a] for a in axes[:stage - 1]}
        away[axis] = 1 - bits[axis]
        dst = bufs[stage].at[(slice(None),) * (3 - stage) + (pl.ds(*rows), slice(None))]
        return remote(own(view(away, rows)), dst, s, r, axis)

    def rs_step(flow, stage):
        own, _, bufs, rows, axes, _ = flow
        rs_copy(flow, stage).wait()
        ref = own(view({a: bits[a] for a in axes[:stage]}, rows))
        ref[...] = ref[...] + bufs[stage][(slice(None),) * (3 - stage) + (pl.ds(*rows), slice(None))]
        if stage < 3:
            rs_copy(flow, stage + 1).start()

    def ag_copy(kind, p, rows, slot):
        axes = AXES[p]
        if slot in (0, 1):
            at, axis = dict(home), (3 if slot == 0 else axes[0])
        elif slot in (2, 3):
            at, axis = {a: bits[a] for a in axes[slot - 1:]}, axes[slot - 1]
        else:
            st = slot - 3
            at, axis = {a: bits[a] for a in axes[st:]}, 3
            at[axes[st - 1]] = 1 - bits[axes[st - 1]]
        spot = gat.at[(kind, core) + view(at, rows)]
        return remote(spot, spot, ag_s.at[kind, p, slot], ag_r.at[kind, p, slot], axis)

    flows = [(KIND_X[p], p, (0, PAD)) for p in range(3)]
    flows_y = [(0, p, AG_Y[p]) for p in range(3)]

    def ag_begin(fl):
        ag_copy(*fl, 1).start()
        ag_copy(*fl, 0).start()

    def ag_step(fl, stage):
        ag_copy(*fl, stage).wait()
        if stage < 3:
            ag_copy(*fl, stage + 1).start()
        ag_copy(*fl, 3 + stage).start()

    def ag_end(fl):
        for slot in (0, 4, 5, 6):
            ag_copy(*fl, slot).wait()

    def adam(kind, grad):
        m_i, v_i, m_o, v_o = (mu, vu, mu_o, vu_o) if kind < 2 else (md, vd, md_o, vd_o)
        l = kind % 2
        new_mom, new_var, n = adam_shard(m_i[:, l, :], v_i[:, l, :], grad)
        m_o[:, l, :] = new_mom
        v_o[:, l, :] = new_var
        full = jnp.concatenate([n, jnp.zeros((PAD - SHARD, RANK), F32)], axis=0)
        gat[(kind, core, bits[0], bits[1], bits[2])] = full.astype(BF16)

    def n_copy(kind, slot):
        return pltpu.make_async_copy(nb.at[slot], n_hbm.at[kind], nsem.at[slot])

    def gather_rows(kind, slot):
        for d in range(DEV):
            block = gat[kind, d % 2, d // 8, d // 4 % 2, d // 2 % 2]
            tmp[SHARD * d:SHARD * (d + 1), :] = block.astype(F32)[:SHARD]
        nb[slot] = tmp[...].astype(BF16)
        n_copy(kind, slot).start()

    def local(k):
        src, dst = ((g1_hbm, g1), (u0_hbm, u0), (rx_hbm.at[core], own_x))[k]
        return pltpu.make_async_copy(src, dst, lsem.at[k])

    def begin():
        barrier = pltpu.get_barrier_semaphore()
        for a in range(4):
            pl.semaphore_signal(barrier, inc=1, device_id=(peer[a],), device_id_type=MESH)
        for k in range(3):
            local(k).start()
        pl.semaphore_wait(barrier, 4)
        for h in range(2):
            for p in range(3):
                rs_copy(flow_x(h, p), 0).start()
        local(0).wait()
        local(1).wait()

    def all_x(h, stage):
        for p in range(3):
            rs_step(flow_x(h, p), stage)

    def first_x():
        local(2).wait()
        all_x(0, 0)

    def finish_x():
        all_x(1, 3)
        for p in range(3):
            adam(KIND_X[p], own_x[bits[0], bits[1], bits[2], p * PAD:p * PAD + SHARD, :])
            ag_begin(flows[p])

    events = {0: begin, 1: first_x, 2: lambda: all_x(1, 0), 4: lambda: all_x(0, 1), 6: lambda: all_x(1, 1),
              7: lambda: all_x(0, 2), 8: lambda: all_x(1, 2), 9: lambda: all_x(0, 3), 10: finish_x}
    for at, event in events.items():
        pl.when(j == at)(event)

    now = lax.rem(j, 2)

    def turn(step):
        rt[pl.ds(pl.multiple_of(step * width, width), width), :] = racc[lax.rem(step, 2)].T

    def act(t):
        k = t % 2
        for r in range(0, tile, slab):
            slope = gelu_both(z0_ref[t * tile + r:t * tile + r + slab, :])[1]
            dz[k, r:r + slab, :] = (slope * das[k, r:r + slab, :]).astype(BF16)

    def acc(t):
        part = dot_nn(u0[:, t * tile:(t + 1) * tile], dz[t % 2])
        if t == tiles - 1:
            racc[now] = acc_s[...] + part
        else:
            acc_s[...] = part if t == 0 else acc_s[...] + part

    turn(lax.rem(j + chunks - 1, chunks))
    for t in range(tiles + 2):
        if t < tiles:
            das[t % 2] = dot_nt(g1[t * tile:(t + 1) * tile, :], w2_ref[...])
        if 1 <= t <= tiles:
            act(t - 1)
        if t >= 2:
            acc(t - 2)

    @pl.when(j == chunks - 1)
    def _():
        turn(j)
        for d in range(DEV):
            own_y[d % 2, d // 8, d // 4 % 2, d // 2 % 2] = rt[SHARD * d:SHARD * d + PAD, :]
        for p in range(3):
            rs_copy(flow_y(p), 0).start()
        for fl in flows:
            ag_step(fl, 1)
        for p in range(3):
            rs_step(flow_y(p), 0)
        for fl in flows:
            ag_step(fl, 2)
        for stage in (1, 2, 3):
            for p in range(3):
                rs_step(flow_y(p), stage)
        adam(0, own_y[core, bits[0], bits[1], bits[2], 0:SHARD, :])
        for fl in flows_y:
            ag_begin(fl)
        for fl in flows:
            ag_step(fl, 3)
        for fl in flows_y:
            ag_step(fl, 1)
        for p, fl in enumerate(flows):
            ag_end(fl)
            if p == 2:
                n_copy(KIND_X[0], 0).wait()
            gather_rows(KIND_X[p], p % 2)
            for other in flows_y if p < 2 else ():
                ag_step(other, 2 + p)
        for fl in flows_y:
            ag_end(fl)
        n_copy(KIND_X[1], 1).wait()
        gather_rows(0, 1)
        n_copy(KIND_X[2], 0).wait()
        n_copy(0, 1).wait()


def call_d(z0, g1, u0, w2, rx, mu, vu, md, vd):
    rows, tile, width = z0.shape[0], 512, 256
    chunks = FFP // width
    mom = jax.ShapeDtypeStruct((SHARD, 2, RANK), F32)
    momspec = pl.BlockSpec((SHARD, 2, RANK), lambda j: (0, 0, 0), pipeline_mode=ONCE)
    x, y = (2, 2, 2, 3 * PAD, RANK), (2, 2, 2, PAD, RANK)
    dma = pltpu.SemaphoreType.DMA
    return pl.pallas_call(
        functools.partial(kernel_d, tile, rows // tile, width, chunks),
        grid=(chunks,),
        in_specs=[
            pl.BlockSpec((rows, width), lambda j: (0, j)),
            pl.BlockSpec((None, width, D), lambda j: (0, j, 0)),
            momspec, momspec, momspec, momspec, ANY, ANY, ANY,
        ],
        out_specs=[momspec] * 4 + [ANY],
        out_shape=[mom] * 4 + [jax.ShapeDtypeStruct((4, FF, RANK), BF16)],
        scratch_shapes=[
            pltpu.VMEM((rows, D), BF16), pltpu.VMEM((RANK, rows), BF16),
            pltpu.VMEM((2, tile, width), F32), pltpu.VMEM((2, tile, width), BF16),
            pltpu.VMEM((RANK, width), F32), pltpu.VMEM((2, RANK, width), F32), pltpu.VMEM((FFP, RANK), F32),
            pltpu.VMEM(x, F32), pltpu.VMEM(x, F32), pltpu.VMEM(x[1:], F32), pltpu.VMEM(x[2:], F32), pltpu.VMEM(x[3:], F32),
            pltpu.VMEM((2,) + y, F32), pltpu.VMEM(y, F32), pltpu.VMEM(y[1:], F32), pltpu.VMEM(y[2:], F32), pltpu.VMEM(y[3:], F32),
            pltpu.VMEM((4, 2) + y, BF16), pltpu.VMEM((FF, RANK), F32), pltpu.VMEM((2, FF, RANK), BF16),
            dma((3,)), dma((2, 3, 4)), dma((2, 3, 4)), dma((3, 4)), dma((3, 4)), dma((4, 3, 7)), dma((4, 3, 7)), dma((2,)),
        ],
        compiler_params=pltpu.CompilerParams(
            dimension_semantics=("arbitrary",), collective_id=0, has_side_effects=True, vmem_limit_bytes=67000000),
        cost_estimate=pl.CostEstimate(flops=30 * 10**9, bytes_accessed=70 * 10**6, transcendentals=0),
        name="pass_d",
    )(z0, w2, mu, vu, md, vd, g1, u0, rx)


def kernel_w(w_ref, n_ref, p_ref, o_ref):
    n = n_ref[...]
    for s in range(0, D, 256):
        delta = dot_nt(n, p_ref[s:s + 256, :])
        o_ref[:, s:s + 256] = (w_ref[:, s:s + 256].astype(F32) - (LEARN_RATE * ALPHA_SCALE) * delta).astype(BF16)


def call_w(w, n, p, first):
    width = 912
    return pl.pallas_call(
        kernel_w,
        grid=(2, FF // width),
        in_specs=[
            pl.BlockSpec((None, width, D), lambda l, j: (l, j, 0)),
            pl.BlockSpec((None, width, RANK), lambda l, j: (first + l, j, 0)),
            pl.BlockSpec((None, D, RANK), lambda l, j: (l, 0, 0)),
        ],
        out_specs=pl.BlockSpec((None, width, D), lambda l, j: (l, j, 0)),
        out_shape=jax.ShapeDtypeStruct((2, FF, D), BF16),
        compiler_params=pltpu.CompilerParams(dimension_semantics=("arbitrary", "arbitrary")),
        cost_estimate=pl.CostEstimate(flops=3 * 10**9, bytes_accessed=23 * 10**6, transcendentals=0),
        name="pass_w",
    )(w, n, p)


def solution(mesh):
    def local_step(x_loc, dh_loc, w_up, w_down, proj_up, proj_down, mom_up, var_up, mom_down, var_down):
        w_up_t = jnp.swapaxes(w_up, 1, 2)
        z0, g1, u0, rx = call_a(x_loc, dh_loc, proj_up, proj_down, w_up_t, w_down)
        rx = rx.reshape(2, 2, 2, 2, 3 * PAD, RANK)
        up, down = (2, 0, 1), (1, 0, 2)
        mu, vu, md, vd, dirs = call_d(
            z0, g1, u0, w_down, rx, jnp.transpose(mom_up, up), jnp.transpose(var_up, up),
            jnp.transpose(mom_down, down), jnp.transpose(var_down, down))
        new_mom_up, new_var_up = jnp.transpose(mu, (1, 2, 0)), jnp.transpose(vu, (1, 2, 0))
        new_mom_down, new_var_down = jnp.transpose(md, (1, 0, 2)), jnp.transpose(vd, (1, 0, 2))
        new_w_up = jnp.swapaxes(call_w(w_up_t, dirs, proj_up, 0), 1, 2)
        new_w_down = call_w(w_down, dirs, proj_down, 2)
        return new_w_up, new_w_down, new_mom_up, new_var_up, new_mom_down, new_var_down

    tok_spec = P('data', None)
    up_spec = P(None, None, 'data')
    down_spec = P(None, 'data', None)
    return jax.shard_map(
        local_step,
        mesh=mesh,
        in_specs=(tok_spec, tok_spec, P(), P(), P(), P(), up_spec, up_spec, down_spec, down_spec),
        out_specs=(P(), P(), up_spec, up_spec, down_spec, down_spec),
        check_vma=False,
    )
```

```python
import functools

import jax
import jax.numpy as jnp
from jax import lax
from jax.experimental import pallas as pl
from jax.experimental.pallas import tpu as pltpu
from jax.sharding import PartitionSpec as P

BETA_ONE = 0.9
BETA_TWO = 0.999
EPSILON = 1e-8
STEP = 4
LEARN_RATE = 0.02
ALPHA_SCALE = 0.25

C0 = 0.7978845608028654
C1 = C0 * 0.044715
D = 1024
FF = 2736
RANK = 256
DEV = 16
SHARD = FF // DEV
PAD = 176
FFP = DEV * PAD
F32 = jnp.float32
BF16 = jnp.bfloat16


def spans_of(width):
    return [(s, min(width, FF - s)) for s in range(0, FF, width)]


def dot_nn(a, b):
    return lax.dot_general(a, b, (((1,), (0,)), ((), ())), preferred_element_type=F32)


def dot_nt(a, b):
    return lax.dot_general(a, b, (((1,), (1,)), ((), ())), preferred_element_type=F32)


def gelu_val(z):
    z2 = z * z
    t = jnp.tanh(z * (C0 + C1 * z2))
    return z * (0.5 * t + 0.5)


def gelu_both(z):
    z2 = z * z
    t = jnp.tanh(z * (C0 + C1 * z2))
    c = 0.5 * t + 0.5
    a = z * c
    slope = c + (a - a * c) * (2.0 * C0 + 6.0 * C1 * z2)
    return a, slope


ANY = pl.BlockSpec(memory_space=pl.ANY)
ONCE = pl.Buffered(1)


def kernel_a(tile, tiles, x_ref, dh_ref, p_ref, q_ref, w1_hbm, w2_hbm,
             z0_hbm, a0_hbm, dz1, u0_ref, r_hbm,
             w1a, w2a, w1b, w2b, z0, a0, h1, zs, das, ac, u1, v1, r1, r2, blk, sem, zsem):
    i = pl.program_id(0)
    width, slab = 512, 16
    spans = spans_of(width)
    loads = [
        pltpu.make_async_copy(w1_hbm.at[0], w1a, sem.at[0]),
        pltpu.make_async_copy(w2_hbm.at[0], w2a, sem.at[1]),
        pltpu.make_async_copy(w1_hbm.at[1], w1b, sem.at[2]),
        pltpu.make_async_copy(w2_hbm.at[1], w2b, sem.at[3]),
    ]

    def out(idx, k):
        src, dst = ((z0, z0_hbm), (a0, a0_hbm))[k]
        return pltpu.make_async_copy(src, dst.at[pl.ds(pl.multiple_of(idx * tile, tile), tile)], zsem.at[k])

    @pl.when(i == 0)
    def _():
        for cp in loads:
            cp.start()
        r1[...] = jnp.zeros_like(r1)
        r2[...] = jnp.zeros_like(r2)
        for cp in loads:
            cp.wait()

    @pl.when(i > 0)
    def _():
        out(i - 1, 0).wait()
        out(i - 1, 1).wait()

    x = x_ref[...]
    dh = dh_ref[...]

    def act0(span):
        s, w = span
        for r in range(0, tile, slab):
            a0[r:r + slab, s:s + w] = gelu_val(z0[r:r + slab, s:s + w]).astype(BF16)

    prev = None
    for span in spans:
        s, w = span
        z0[:, s:s + w] = dot_nt(x, w1a[s:s + w, :])
        if prev is not None:
            act0(prev)
        prev = span
    u0_ref[...] = dot_nt(p_ref[0], x).astype(BF16)
    v1[...] = dot_nt(q_ref[1], dh).astype(BF16)
    act0(prev)

    for n in range(0, D, width):
        h1[:, n:n + width] = (x_ref[:, n:n + width].astype(F32) + dot_nn(a0[...], w2a[:, n:n + width])).astype(BF16)
    out(i, 0).start()
    out(i, 1).start()

    def act1(span, k):
        s, w = span
        for r in range(0, tile, slab):
            a, g = gelu_both(zs[k, r:r + slab, :w])
            ac[k, r:r + slab, :w] = a.astype(BF16)
            dz1[r:r + slab, s:s + w] = (g * das[k, r:r + slab, :w]).astype(BF16)

    def acc1(span, k):
        s, w = span
        r2[:, s:s + w] += dot_nn(v1[...], ac[k, :, :w])
        r1[:, s:s + w] += dot_nn(u1[...], dz1[:, s:s + w])

    h = h1[...]
    n = len(spans)
    for j in range(n + 2):
        if j < n:
            s, w = spans[j]
            das[j % 2, :, :w] = dot_nt(dh, w2b[s:s + w, :])
            zs[j % 2, :, :w] = dot_nt(h, w1b[s:s + w, :])
        if j == 0:
            u1[...] = dot_nt(p_ref[1], h).astype(BF16)
        if 1 <= j <= n:
            act1(spans[j - 1], (j - 1) % 2)
        if j >= 2:
            acc1(spans[j - 2], (j - 2) % 2)

    @pl.when(i == tiles - 1)
    def _():
        out(i, 0).wait()
        out(i, 1).wait()
        for k, acc in enumerate((r1, r2)):
            for t in range(FFP // 256):
                z0[t % 2 * 256:t % 2 * 256 + 256, t // 2 * 256:t // 2 * 256 + 256] = acc[:, t * 256:t * 256 + 256].T
            if k == 1:
                pltpu.make_async_copy(blk, r_hbm.at[0], sem.at[0]).wait()
            for d in range(DEV):
                row, end = SHARD * d, SHARD * d + PAD
                while row < end:
                    t, lo = row // 256, row % 256
                    take = min(end - row, 256 - lo)
                    to = row - SHARD * d
                    blk[(d % 2) * 8 + d // 2, to:to + take, :] = z0[t % 2 * 256 + lo:t % 2 * 256 + lo + take, t // 2 * 256:t // 2 * 256 + 256]
                    row += take
            pltpu.make_async_copy(blk, r_hbm.at[k], sem.at[k]).start()
        pltpu.make_async_copy(blk, r_hbm.at[1], sem.at[1]).wait()


def leave(acc, rt):
    for s in range(0, FFP, 256):
        rt[s:s + 256, :] = acc[:, s:s + 256].T


def call_a(x, dh, p, q, w1, w2):
    rows, tile = x.shape[0], 512
    tiles = rows // tile
    whole = pl.BlockSpec((2, RANK, D), lambda i: (0, 0, 0), pipeline_mode=ONCE)
    rowspec = pl.BlockSpec((tile, D), lambda i: (i, 0))
    return pl.pallas_call(
        functools.partial(kernel_a, tile, tiles),
        grid=(tiles,),
        in_specs=[rowspec, rowspec, whole, whole, ANY, ANY],
        out_specs=[ANY, ANY, pl.BlockSpec((tile, FF), lambda i: (i, 0)), pl.BlockSpec((RANK, tile), lambda i: (0, i)), ANY],
        out_shape=[
            jax.ShapeDtypeStruct((rows, FF), F32),
            jax.ShapeDtypeStruct((rows, FF), BF16),
            jax.ShapeDtypeStruct((rows, FF), BF16),
            jax.ShapeDtypeStruct((RANK, rows), BF16),
            jax.ShapeDtypeStruct((2, DEV, PAD, RANK), F32),
        ],
        scratch_shapes=[
            pltpu.VMEM((FF, D), BF16), pltpu.VMEM((FF, D), BF16),
            pltpu.VMEM((FF, D), BF16), pltpu.VMEM((FF, D), BF16),
            pltpu.VMEM((tile, FF), F32), pltpu.VMEM((tile, FF), BF16), pltpu.VMEM((tile, D), BF16),
            pltpu.VMEM((2, tile, 512), F32), pltpu.VMEM((2, tile, 512), F32), pltpu.VMEM((2, tile, 512), BF16),
            pltpu.VMEM((RANK, tile), BF16), pltpu.VMEM((RANK, tile), BF16),
            pltpu.VMEM((RANK, FFP), F32), pltpu.VMEM((RANK, FFP), F32),
            pltpu.VMEM((DEV, PAD, RANK), F32),
            pltpu.SemaphoreType.DMA((4,)), pltpu.SemaphoreType.DMA((2,)),
        ],
        compiler_params=pltpu.CompilerParams(
            dimension_semantics=("arbitrary",), vmem_limit_bytes=67000000),
        cost_estimate=pl.CostEstimate(flops=110 * 10**9, bytes_accessed=140 * 10**6, transcendentals=0),
        name="pass_a",
    )(x, dh, p, q, w1, w2)


def adam_shard(moment, variance, grad_red):
    new_mom = BETA_ONE * moment + (1.0 - BETA_ONE) * grad_red
    new_var = BETA_TWO * variance + (1.0 - BETA_TWO) * grad_red * grad_red
    bias_one = 1.0 - BETA_ONE ** STEP
    bias_two = 1.0 - BETA_TWO ** STEP
    direction = (new_mom / bias_one) / (jnp.sqrt(new_var / bias_two) + EPSILON)
    return new_mom, new_var, direction


AXES = ((2, 1, 0), (1, 0, 2), (0, 2, 1))
RS_ROWS = ((0, 56), (56, 56), (112, 64))
AG_ROWS = ((0, 48), (48, 64), (112, 64))
MESH = pl.DeviceIdType.MESH
CUBE = (2, 2, 2, PAD, RANK)


def view(fixed, rows):
    return tuple(fixed.get(a, slice(None)) for a in range(3)) + (pl.ds(*rows), slice(None))


class Comm:
    def __init__(self):
        me = lax.axis_index('data')
        self.bits = [lax.rem(me // (8 >> a), 2) for a in range(4)]
        self.peer = [me + (1 - 2 * self.bits[a]) * (8 >> a) for a in range(4)]
        self.core = self.bits[3]

    def greet(self):
        barrier = pltpu.get_barrier_semaphore()
        for a in range(4):
            pl.semaphore_signal(barrier, inc=1, device_id=(self.peer[a],), device_id_type=MESH)

    def met(self):
        pl.semaphore_wait(pltpu.get_barrier_semaphore(), 4)

    def remote(self, src, dst, s, r, axis):
        return pltpu.make_async_remote_copy(src_ref=src, dst_ref=dst, send_sem=s, recv_sem=r,
                                            device_id=(self.peer[axis],), device_id_type=MESH)

    def rs_copy(self, flow, stage):
        own, other, bufs, sems, p = flow
        rows, axes = RS_ROWS[p], AXES[p]
        s, r = (sem.at[p, stage] for sem in sems)
        if stage == 0:
            spot = view({}, rows)
            return self.remote(other.at[spot], bufs[0].at[spot], s, r, 3)
        axis = axes[stage - 1]
        away = {a: self.bits[a] for a in axes[:stage - 1]}
        away[axis] = 1 - self.bits[axis]
        dst = bufs[stage].at[(slice(None),) * (3 - stage) + (pl.ds(*rows), slice(None))]
        return self.remote(own.at[view(away, rows)], dst, s, r, axis)

    def rs_step(self, flow, stage):
        own, _, bufs, _, p = flow
        rows, axes = RS_ROWS[p], AXES[p]
        self.rs_copy(flow, stage).wait()
        ref = own.at[view({a: self.bits[a] for a in axes[:stage]}, rows)]
        ref[...] = ref[...] + bufs[stage][(slice(None),) * (3 - stage) + (pl.ds(*rows), slice(None))]
        if stage < 3:
            self.rs_copy(flow, stage + 1).start()

    def ag_copy(self, gat, sems, kind, p, slot):
        rows, axes, bits = AG_ROWS[p], AXES[p], self.bits
        if slot == 0:
            at, axis = {a: bits[a] for a in range(3)}, 3
        elif slot <= 3:
            at, axis = {a: bits[a] for a in axes[slot - 1:]}, axes[slot - 1]
        else:
            at, axis = {a: bits[a] for a in axes[slot - 3:]}, 3
            at[axes[slot - 4]] = 1 - bits[axes[slot - 4]]
        spot = gat.at[(kind, self.core) + view(at, rows)]
        return self.remote(spot, spot, sems[0].at[kind, p, slot], sems[1].at[kind, p, slot], axis)

    def ag_begin(self, *flow):
        self.ag_copy(*flow, 1).start()
        self.ag_copy(*flow, 0).start()

    def ag_step(self, *flow, stage):
        self.ag_copy(*flow, stage).wait()
        if stage < 3:
            self.ag_copy(*flow, stage + 1).start()
        self.ag_copy(*flow, 3 + stage).start()

    def ag_end(self, *flow):
        for slot in (0, 4, 5, 6):
            self.ag_copy(*flow, slot).wait()


def stages():
    return [pltpu.VMEM(CUBE[k:], F32) if k else pltpu.VMEM(CUBE, F32) for k in range(4)]


def kernel_c(tile, tiles, dh_ref, dz_ref, a0_ref, w1_ref, q_ref, rx_hbm,
             g1_ref, sum_ref, ry_hbm,
             r3, rt, blk, own, xa0, xa1, xa2, xa3, xb0, xb1, xb2, xb3, lsem, as_, ar, bs, br):
    i = pl.program_id(0)
    c = Comm()
    bufs = ((xa0, xa1, xa2, xa3), (xb0, xb1, xb2, xb3))
    sems = ((as_, ar), (bs, br))
    flows = [(own.at[k], rx_hbm.at[k, 1 - c.core], bufs[k], sems[k], p) for k in range(2) for p in range(3)]

    def mine():
        return pltpu.make_async_copy(rx_hbm.at[:, c.core], own, lsem.at[0])

    @pl.when(i == 0)
    def _():
        c.greet()
        mine().start()
        r3[...] = jnp.zeros_like(r3)
        c.met()
        for flow in flows:
            c.rs_copy(flow, 0).start()

    @pl.when(i == 2)
    def _():
        mine().wait()

    for at, stage in ((2, 0), (5, 1), (7, 2)):
        @pl.when(i == at)
        def _():
            for flow in flows:
                c.rs_step(flow, stage)

    half = 512
    for n in range(0, D, half):
        g1_ref[:, n:n + half] = (dh_ref[:, n:n + half].astype(F32) + dot_nn(dz_ref[...], w1_ref[:, n:n + half])).astype(BF16)
    v0 = dot_nt(q_ref[...], g1_ref[...]).astype(BF16)
    for s, w in spans_of(512):
        r3[:, s:s + w] += dot_nn(v0, a0_ref[:, s:s + w])

    @pl.when(i == tiles - 1)
    def _():
        leave(r3, rt)
        for d in range(DEV):
            blk[(d % 2) * 8 + d // 2] = rt[SHARD * d:SHARD * d + PAD, :]
        out = pltpu.make_async_copy(blk, ry_hbm, lsem.at[0])
        out.start()
        for flow in flows:
            c.rs_step(flow, 3)
        for k in range(2):
            sum_ref[k] = own[k, c.bits[0], c.bits[1], c.bits[2]]
        out.wait()


def call_c(dh, dz, a0, w1, q, rx):
    rows, tile = dh.shape[0], 512
    tiles = rows // tile
    dma = pltpu.SemaphoreType.DMA
    return pl.pallas_call(
        functools.partial(kernel_c, tile, tiles),
        grid=(tiles,),
        in_specs=[
            pl.BlockSpec((tile, D), lambda i: (i, 0)),
            pl.BlockSpec((tile, FF), lambda i: (i, 0)),
            pl.BlockSpec((tile, FF), lambda i: (i, 0)),
            pl.BlockSpec((None, FF, D), lambda i: (1, 0, 0), pipeline_mode=ONCE),
            pl.BlockSpec((None, RANK, D), lambda i: (0, 0, 0), pipeline_mode=ONCE),
            ANY,
        ],
        out_specs=[
            pl.BlockSpec((tile, D), lambda i: (i, 0)),
            pl.BlockSpec((2, PAD, RANK), lambda i: (0, 0, 0), pipeline_mode=ONCE),
            ANY,
        ],
        out_shape=[
            jax.ShapeDtypeStruct((rows, D), BF16),
            jax.ShapeDtypeStruct((2, PAD, RANK), F32),
            jax.ShapeDtypeStruct((DEV, PAD, RANK), F32),
        ],
        scratch_shapes=[
            pltpu.VMEM((RANK, FFP), F32), pltpu.VMEM((FFP, RANK), F32), pltpu.VMEM((DEV, PAD, RANK), F32),
            pltpu.VMEM((2,) + CUBE, F32), *stages(), *stages(),
            dma((1,)), dma((3, 4)), dma((3, 4)), dma((3, 4)), dma((3, 4)),
        ],
        compiler_params=pltpu.CompilerParams(
            dimension_semantics=("arbitrary",), collective_id=1, has_side_effects=True, vmem_limit_bytes=60000000),
        cost_estimate=pl.CostEstimate(flops=31 * 10**9, bytes_accessed=70 * 10**6, transcendentals=0),
        name="pass_c",
    )(dh, dz, a0, w1, q, rx)


def kernel_d(tile, tiles, width, chunks,
             z0_ref, w2_ref, sum_ref, mu, vu, md, vd, g1_hbm, u0_hbm, rx_hbm,
             mu_o, vu_o, md_o, vd_o, n_hbm,
             g1, u0, das, dz, acc_s, racc, rt, own_x, own_y,
             x0, x1, x2, x3, y0, y1, y2, y3, gat, tmp, nb,
             lsem, rx_s, rx_r, ry_s, ry_r, ag_s, ag_r, nsem):
    j = pl.program_id(0)
    slab = 16
    c = Comm()
    bits, core = c.bits, c.core
    ag_sems = (ag_s, ag_r)
    flows_x = [(own_x, rx_hbm.at[1 - core], (x0, x1, x2, x3), (rx_s, rx_r), p) for p in range(3)]
    flows_y = [(own_y.at[core], own_y.at[1 - core], (y0, y1, y2, y3), (ry_s, ry_r), p) for p in range(3)]

    def rs(flows, stage):
        for flow in flows:
            c.rs_step(flow, stage)

    def ag(kinds, stage):
        for kind in kinds:
            for p in range(3):
                if stage == 0:
                    c.ag_begin(gat, ag_sems, kind, p)
                elif stage < 4:
                    c.ag_step(gat, ag_sems, kind, p, stage=stage)
                else:
                    c.ag_end(gat, ag_sems, kind, p)

    def adam(kind, grad):
        m_i, v_i, m_o, v_o = (mu, vu, mu_o, vu_o) if kind < 2 else (md, vd, md_o, vd_o)
        l = kind % 2
        new_mom, new_var, n = adam_shard(m_i[:, l, :], v_i[:, l, :], grad)
        m_o[:, l, :] = new_mom
        v_o[:, l, :] = new_var
        full = jnp.concatenate([n, jnp.zeros((PAD - SHARD, RANK), F32)], axis=0)
        gat[(kind, core, bits[0], bits[1], bits[2])] = full.astype(BF16)

    def n_copy(kind):
        return pltpu.make_async_copy(nb.at[kind % 2], n_hbm.at[kind], nsem.at[kind])

    def gather_rows(kind):
        for d in range(DEV):
            block = gat[kind, d % 2, d // 8, d // 4 % 2, d // 2 % 2]
            tmp[SHARD * d:SHARD * (d + 1), :] = block.astype(F32)[:SHARD]
        nb[kind % 2] = tmp[...].astype(BF16)
        n_copy(kind).start()

    def local(k):
        src, dst = ((g1_hbm, g1), (u0_hbm, u0), (rx_hbm.at[core], own_x))[k]
        return pltpu.make_async_copy(src, dst, lsem.at[k])

    def begin():
        c.greet()
        for k in range(3):
            local(k).start()
        adam(1, sum_ref[0, 0:SHARD, :])
        adam(3, sum_ref[1, 0:SHARD, :])
        c.met()
        ag((1, 3), 0)
        for flow in flows_x:
            c.rs_copy(flow, 0).start()
        for k in range(3):
            local(k).wait()

    def step_one():
        rs(flows_x, 0)
        ag((1, 3), 1)

    def finish_x():
        rs(flows_x, 3)
        adam(2, own_x[bits[0], bits[1], bits[2], 0:SHARD, :])
        ag((2,), 0)

    events = {0: begin, 1: step_one, 2: lambda: ag((1, 3), 2), 3: lambda: rs(flows_x, 1), 4: lambda: ag((1, 3), 3),
              5: lambda: rs(flows_x, 2), 7: finish_x, 8: lambda: ag((2,), 1), 9: lambda: ag((2,), 2), 10: lambda: ag((2,), 3)}
    for at, event in events.items():
        pl.when(j == at)(event)

    now = lax.rem(j, 2)

    def turn(step):
        rt[pl.ds(pl.multiple_of(step * width, width), width), :] = racc[lax.rem(step, 2)].T

    def act(t):
        k = t % 2
        for r in range(0, tile, slab):
            slope = gelu_both(z0_ref[t * tile + r:t * tile + r + slab, :])[1]
            dz[k, r:r + slab, :] = (slope * das[k, r:r + slab, :]).astype(BF16)

    def acc(t):
        part = dot_nn(u0[:, t * tile:(t + 1) * tile], dz[t % 2])
        if t == tiles - 1:
            racc[now] = acc_s[...] + part
        else:
            acc_s[...] = part if t == 0 else acc_s[...] + part

    turn(lax.rem(j + chunks - 1, chunks))
    for t in range(tiles + 2):
        if t < tiles:
            das[t % 2] = dot_nt(g1[t * tile:(t + 1) * tile, :], w2_ref[...])
        if 1 <= t <= tiles:
            act(t - 1)
        if t >= 2:
            acc(t - 2)

    @pl.when(j == chunks - 1)
    def _():
        turn(j)
        for d in range(DEV):
            own_y[d % 2, d // 8, d // 4 % 2, d // 2 % 2] = rt[SHARD * d:SHARD * d + PAD, :]
        for flow in flows_y:
            c.rs_copy(flow, 0).start()
        ag((1, 3), 4)
        gather_rows(1)
        rs(flows_y, 0)
        ag((2,), 4)
        gather_rows(2)
        rs(flows_y, 1)
        n_copy(1).wait()
        gather_rows(3)
        rs(flows_y, 2)
        rs(flows_y, 3)
        adam(0, own_y[core, bits[0], bits[1], bits[2], 0:SHARD, :])
        for stage in range(5):
            ag((0,), stage)
        n_copy(2).wait()
        gather_rows(0)
        n_copy(3).wait()
        n_copy(0).wait()


def call_d(z0, g1, u0, w2, sums, rx, mu, vu, md, vd):
    rows, tile, width = z0.shape[0], 512, 256
    chunks = FFP // width
    mom = jax.ShapeDtypeStruct((SHARD, 2, RANK), F32)
    momspec = pl.BlockSpec((SHARD, 2, RANK), lambda j: (0, 0, 0), pipeline_mode=ONCE)
    dma = pltpu.SemaphoreType.DMA
    return pl.pallas_call(
        functools.partial(kernel_d, tile, rows // tile, width, chunks),
        grid=(chunks,),
        in_specs=[
            pl.BlockSpec((rows, width), lambda j: (0, j)),
            pl.BlockSpec((None, width, D), lambda j: (0, j, 0)),
            pl.BlockSpec((2, PAD, RANK), lambda j: (0, 0, 0), pipeline_mode=ONCE),
            momspec, momspec, momspec, momspec, ANY, ANY, ANY,
        ],
        out_specs=[momspec] * 4 + [ANY],
        out_shape=[mom] * 4 + [jax.ShapeDtypeStruct((4, FF, RANK), BF16)],
        scratch_shapes=[
            pltpu.VMEM((rows, D), BF16), pltpu.VMEM((RANK, rows), BF16),
            pltpu.VMEM((2, tile, width), F32), pltpu.VMEM((2, tile, width), BF16),
            pltpu.VMEM((RANK, width), F32), pltpu.VMEM((2, RANK, width), F32), pltpu.VMEM((FFP, RANK), F32),
            pltpu.VMEM(CUBE, F32), pltpu.VMEM((2,) + CUBE, F32), *stages(), *stages(),
            pltpu.VMEM((4, 2) + CUBE, BF16), pltpu.VMEM((FF, RANK), F32), pltpu.VMEM((2, FF, RANK), BF16),
            dma((3,)), dma((3, 4)), dma((3, 4)), dma((3, 4)), dma((3, 4)), dma((4, 3, 7)), dma((4, 3, 7)), dma((4,)),
        ],
        compiler_params=pltpu.CompilerParams(
            dimension_semantics=("arbitrary",), collective_id=0, has_side_effects=True, vmem_limit_bytes=67000000),
        cost_estimate=pl.CostEstimate(flops=30 * 10**9, bytes_accessed=70 * 10**6, transcendentals=0),
        name="pass_d",
    )(z0, w2, sums, mu, vu, md, vd, g1, u0, rx)


def kernel_w(count, part, wu_hbm, wd_hbm, n_hbm, p_ref, q_ref, nu_hbm, nd_hbm, buf, n, isem, nsem, osem):
    per = FF // part

    def load(k):
        src, at = (wu_hbm, k) if k < 2 * per else (wd_hbm, k - 2 * per)
        return pltpu.make_async_copy(src.at[at], buf.at[k], isem.at[k])

    def names(kind):
        return pltpu.make_async_copy(n_hbm.at[pl.ds(kind * per, per)], n.at[pl.ds(kind * per, per)], nsem.at[kind])

    for k in range(count):
        if k % per == 0:
            names(k // per).start()
        load(k).start()
    for kind in range(4):
        proj, dst, base = (p_ref, nu_hbm, 0) if kind < 2 else (q_ref, nd_hbm, 2 * per)
        names(kind).wait()

        def body(t, carry):
            k = kind * per + t
            pltpu.make_async_copy(wu_hbm.at[0], buf.at[k], isem.at[k]).wait()
            for s in range(0, D, 256):
                delta = dot_nt(n[k], proj[kind % 2, s:s + 256, :])
                buf[k, :, s:s + 256] = (buf[k, :, s:s + 256].astype(F32) - (LEARN_RATE * ALPHA_SCALE) * delta).astype(BF16)
            pltpu.make_async_copy(buf.at[k], dst.at[k - base], osem.at[k]).start()
            return carry

        lax.fori_loop(0, per, body, 0)
    for k in range(count):
        dst, at = (nu_hbm, k) if k < 2 * per else (nd_hbm, k - 2 * per)
        pltpu.make_async_copy(buf.at[k], dst.at[at], osem.at[k]).wait()


def call_w(wu, wd, n, p, q):
    part = 456
    per = FF // part
    count = 4 * per
    whole = pl.BlockSpec(memory_space=pltpu.VMEM)
    out = jax.ShapeDtypeStruct((2 * per, part, D), BF16)
    dma = pltpu.SemaphoreType.DMA
    nu, nd = pl.pallas_call(
        functools.partial(kernel_w, count, part),
        in_specs=[ANY, ANY, ANY, whole, whole],
        out_specs=[ANY, ANY],
        out_shape=[out, out],
        scratch_shapes=[pltpu.VMEM((count, part, D), BF16), pltpu.VMEM((count, part, RANK), BF16), dma((count,)), dma((4,)), dma((count,))],
        compiler_params=pltpu.CompilerParams(vmem_limit_bytes=60000000),
        cost_estimate=pl.CostEstimate(flops=6 * 10**9, bytes_accessed=50 * 10**6, transcendentals=0),
        name="pass_w",
    )(wu.reshape(2 * per, part, D), wd.reshape(2 * per, part, D), n.reshape(count, part, RANK), p, q)
    return nu.reshape(2, FF, D), nd.reshape(2, FF, D)


def solution(mesh):
    def local_step(x_loc, dh_loc, w_up, w_down, proj_up, proj_down, mom_up, var_up, mom_down, var_down):
        w_up_t = jnp.swapaxes(w_up, 1, 2)
        pt, qt = jnp.swapaxes(proj_up, 1, 2), jnp.swapaxes(proj_down, 1, 2)
        z0, a0, dz1, u0, rx = call_a(x_loc, dh_loc, pt, qt, w_up_t, w_down)
        g1, sums, ry = call_c(dh_loc, dz1, a0, w_up_t, qt, rx.reshape((2, 2) + CUBE))
        up, down = (2, 0, 1), (1, 0, 2)
        mu, vu, md, vd, dirs = call_d(
            z0, g1, u0, w_down, sums, ry.reshape((2,) + CUBE), jnp.transpose(mom_up, up), jnp.transpose(var_up, up),
            jnp.transpose(mom_down, down), jnp.transpose(var_down, down))
        new_mom_up, new_var_up = jnp.transpose(mu, (1, 2, 0)), jnp.transpose(vu, (1, 2, 0))
        new_mom_down, new_var_down = jnp.transpose(md, (1, 0, 2)), jnp.transpose(vd, (1, 0, 2))
        new_up, new_w_down = call_w(w_up_t, w_down, dirs, proj_up, proj_down)
        return jnp.swapaxes(new_up, 1, 2), new_w_down, new_mom_up, new_var_up, new_mom_down, new_var_down

    tok_spec = P('data', None)
    up_spec = P(None, None, 'data')
    down_spec = P(None, 'data', None)
    return jax.shard_map(
        local_step,
        mesh=mesh,
        in_specs=(tok_spec, tok_spec, P(), P(), P(), P(), up_spec, up_spec, down_spec, down_spec),
        out_specs=(P(), P(), up_spec, up_spec, down_spec, down_spec),
        check_vma=False,
    )
```

```python
import functools

import jax
import jax.numpy as jnp
from jax import lax
from jax.experimental import pallas as pl
from jax.experimental.pallas import tpu as pltpu
from jax.sharding import PartitionSpec as P

BETA_ONE = 0.9
BETA_TWO = 0.999
EPSILON = 1e-8
STEP = 4
LEARN_RATE = 0.02
ALPHA_SCALE = 0.25

C0 = 0.7978845608028654
C1 = C0 * 0.044715
D = 1024
FF = 2736
RANK = 256
DEV = 16
SHARD = FF // DEV
PAD = 176
FFP = DEV * PAD
F32 = jnp.float32
BF16 = jnp.bfloat16


def spans_of(width):
    return [(s, min(width, FF - s)) for s in range(0, FF, width)]


def pieces(span, width=256):
    s, w = span
    return [(t, min(width, s + w - t)) for t in range(s, s + w, width)]


def dot_nn(a, b):
    return lax.dot_general(a, b, (((1,), (0,)), ((), ())), preferred_element_type=F32)


def dot_nt(a, b):
    return lax.dot_general(a, b, (((1,), (1,)), ((), ())), preferred_element_type=F32)


def dot_tt(a, b):
    return lax.dot_general(a, b, (((0,), (1,)), ((), ())), preferred_element_type=F32)


def gelu_both(z):
    z2 = z * z
    t = jnp.tanh(z * (C0 + C1 * z2))
    c = 0.5 * t + 0.5
    a = z * c
    slope = c + (a - a * c) * (2.0 * C0 + 6.0 * C1 * z2)
    return a, slope


ANY = pl.BlockSpec(memory_space=pl.ANY)
ONCE = pl.Buffered(1)


def kernel_a(tile, tiles, x_ref, dh_ref, p_ref, q_ref, w1_hbm, w2_hbm,
             slope_hbm, a0_hbm, dz1, u0_ref, r_hbm,
             w1a, w2a, w1b, w2b, slope, a0, h1, zs, das, ac, u1, v1, r1, r2, blk, sem, zsem):
    i = pl.program_id(0)
    width, slab = 512, 16
    spans = spans_of(width)
    loads = [
        pltpu.make_async_copy(w1_hbm.at[0], w1a, sem.at[0]),
        pltpu.make_async_copy(w2_hbm.at[0], w2a, sem.at[1]),
        pltpu.make_async_copy(w1_hbm.at[1], w1b, sem.at[2]),
        pltpu.make_async_copy(w2_hbm.at[1], w2b, sem.at[3]),
    ]

    def out(idx, k):
        src, dst = ((slope, slope_hbm), (a0, a0_hbm))[k]
        return pltpu.make_async_copy(src, dst.at[pl.ds(pl.multiple_of(idx * tile, tile), tile)], zsem.at[k])

    @pl.when(i == 0)
    def _():
        for cp in loads:
            cp.start()
        r1[...] = jnp.zeros_like(r1)
        r2[...] = jnp.zeros_like(r2)
        for cp in loads:
            cp.wait()

    @pl.when(i > 0)
    def _():
        out(i - 1, 0).wait()
        out(i - 1, 1).wait()

    x = x_ref[...]
    dh = dh_ref[...]

    def act0(span, k):
        for s, w in pieces(span):
            o = s - span[0]
            for r in range(0, tile, slab):
                a, g = gelu_both(zs[k, r:r + slab, o:o + w])
                a0[r:r + slab, s:s + w] = a.astype(BF16)
                slope[r:r + slab, s:s + w] = g

    n = len(spans)
    for j in range(n + 1):
        if j < n:
            s, w = spans[j]
            zs[j % 2, :, :w] = dot_nt(x, w1a[s:s + w, :])
        else:
            u0_ref[...] = dot_tt(p_ref[0], x).astype(BF16)
            v1[...] = dot_tt(q_ref[1], dh).astype(BF16)
        if j > 0:
            act0(spans[j - 1], (j - 1) % 2)

    for n in range(0, D, width):
        h1[:, n:n + width] = (x_ref[:, n:n + width].astype(F32) + dot_nn(a0[...], w2a[:, n:n + width])).astype(BF16)
    out(i, 0).start()
    out(i, 1).start()

    def act1(span, k):
        for s, w in pieces(span):
            o = s - span[0]
            for r in range(0, tile, slab):
                a, g = gelu_both(zs[k, r:r + slab, o:o + w])
                ac[k, r:r + slab, o:o + w] = a.astype(BF16)
                dz1[r:r + slab, s:s + w] = (g * das[k, r:r + slab, o:o + w]).astype(BF16)

    def acc1(span, k):
        s, w = span
        r2[:, s:s + w] += dot_nn(v1[...], ac[k, :, :w])
        r1[:, s:s + w] += dot_nn(u1[...], dz1[:, s:s + w])

    h = h1[...]
    n = len(spans)
    for j in range(n + 2):
        if j < n:
            s, w = spans[j]
            das[j % 2, :, :w] = dot_nt(dh, w2b[s:s + w, :])
            zs[j % 2, :, :w] = dot_nt(h, w1b[s:s + w, :])
        if j == 0:
            u1[...] = dot_tt(p_ref[1], h).astype(BF16)
        if 1 <= j <= n:
            act1(spans[j - 1], (j - 1) % 2)
        if j >= 2:
            acc1(spans[j - 2], (j - 2) % 2)

    @pl.when(i == tiles - 1)
    def _():
        out(i, 0).wait()
        out(i, 1).wait()
        for k, acc in enumerate((r1, r2)):
            for t in range(FFP // 256):
                slope[t % 2 * 256:t % 2 * 256 + 256, t // 2 * 256:t // 2 * 256 + 256] = acc[:, t * 256:t * 256 + 256].T
            if k == 1:
                pltpu.make_async_copy(blk, r_hbm.at[0], sem.at[0]).wait()
            for d in range(DEV):
                row, end = SHARD * d, SHARD * d + PAD
                while row < end:
                    t, lo = row // 256, row % 256
                    take = min(end - row, 256 - lo)
                    to = row - SHARD * d
                    blk[(d % 2) * 8 + d // 2, to:to + take, :] = slope[t % 2 * 256 + lo:t % 2 * 256 + lo + take, t // 2 * 256:t // 2 * 256 + 256]
                    row += take
            pltpu.make_async_copy(blk, r_hbm.at[k], sem.at[k]).start()
        pltpu.make_async_copy(blk, r_hbm.at[1], sem.at[1]).wait()


def leave(acc, rt):
    for s in range(0, FFP, 256):
        rt[s:s + 256, :] = acc[:, s:s + 256].T


def call_a(x, dh, p, q, w1, w2):
    rows, tile = x.shape[0], 512
    tiles = rows // tile
    whole = pl.BlockSpec((2, D, RANK), lambda i: (0, 0, 0), pipeline_mode=ONCE)
    rowspec = pl.BlockSpec((tile, D), lambda i: (i, 0))
    return pl.pallas_call(
        functools.partial(kernel_a, tile, tiles),
        grid=(tiles,),
        in_specs=[rowspec, rowspec, whole, whole, ANY, ANY],
        out_specs=[ANY, ANY, pl.BlockSpec((tile, FF), lambda i: (i, 0)), pl.BlockSpec((RANK, tile), lambda i: (0, i)), ANY],
        out_shape=[
            jax.ShapeDtypeStruct((rows, FF), F32),
            jax.ShapeDtypeStruct((rows, FF), BF16),
            jax.ShapeDtypeStruct((rows, FF), BF16),
            jax.ShapeDtypeStruct((RANK, rows), BF16),
            jax.ShapeDtypeStruct((2, DEV, PAD, RANK), F32),
        ],
        scratch_shapes=[
            pltpu.VMEM((FF, D), BF16), pltpu.VMEM((FF, D), BF16),
            pltpu.VMEM((FF, D), BF16), pltpu.VMEM((FF, D), BF16),
            pltpu.VMEM((tile, FF), F32), pltpu.VMEM((tile, FF), BF16), pltpu.VMEM((tile, D), BF16),
            pltpu.VMEM((2, tile, 512), F32), pltpu.VMEM((2, tile, 512), F32), pltpu.VMEM((2, tile, 512), BF16),
            pltpu.VMEM((RANK, tile), BF16), pltpu.VMEM((RANK, tile), BF16),
            pltpu.VMEM((RANK, FFP), F32), pltpu.VMEM((RANK, FFP), F32),
            pltpu.VMEM((DEV, PAD, RANK), F32),
            pltpu.SemaphoreType.DMA((4,)), pltpu.SemaphoreType.DMA((2,)),
        ],
        compiler_params=pltpu.CompilerParams(
            dimension_semantics=("arbitrary",), vmem_limit_bytes=67000000),
        cost_estimate=pl.CostEstimate(flops=110 * 10**9, bytes_accessed=140 * 10**6, transcendentals=0),
        name="pass_a",
    )(x, dh, p, q, w1, w2)


def adam_shard(moment, variance, grad_red):
    new_mom = BETA_ONE * moment + (1.0 - BETA_ONE) * grad_red
    new_var = BETA_TWO * variance + (1.0 - BETA_TWO) * grad_red * grad_red
    bias_one = 1.0 - BETA_ONE ** STEP
    bias_two = 1.0 - BETA_TWO ** STEP
    direction = (new_mom / bias_one) / (jnp.sqrt(new_var / bias_two) + EPSILON)
    return new_mom, new_var, direction


AHEAD = 10
AXES = ((2, 1, 0), (1, 0, 2), (0, 2, 1))
RS_ROWS = ((0, 56), (56, 56), (112, 64), (0, 24), (56, 24), (112, 32), (24, 32), (80, 32), (144, 32))
AG_ROWS = ((0, 48), (48, 64), (112, 64), (0, 16), (48, 32), (112, 32), (16, 32), (80, 32), (144, 32))
THIRDS, SIXTHS = range(3), range(3, 9)
MESH = pl.DeviceIdType.MESH
CUBE = (2, 2, 2, PAD, RANK)


def view(fixed, rows):
    return tuple(fixed.get(a, slice(None)) for a in range(3)) + (pl.ds(*rows), slice(None))


class Comm:
    def __init__(self):
        me = lax.axis_index('data')
        self.bits = [lax.rem(me // (8 >> a), 2) for a in range(4)]
        self.peer = [me + (1 - 2 * self.bits[a]) * (8 >> a) for a in range(4)]
        self.core = self.bits[3]

    def greet(self):
        barrier = pltpu.get_barrier_semaphore()
        for a in range(4):
            pl.semaphore_signal(barrier, inc=1, device_id=(self.peer[a],), device_id_type=MESH)

    def met(self):
        pl.semaphore_wait(pltpu.get_barrier_semaphore(), 4)

    def remote(self, src, dst, s, r, axis):
        return pltpu.make_async_remote_copy(src_ref=src, dst_ref=dst, send_sem=s, recv_sem=r,
                                            device_id=(self.peer[axis],), device_id_type=MESH)

    def rs_copy(self, flow, stage):
        own, other, bufs, sems, p = flow
        rows, axes = RS_ROWS[p], AXES[p % 3]
        s, r = (sem.at[p, stage] for sem in sems)
        if stage == 0:
            spot = view({}, rows)
            return self.remote(other.at[spot], bufs[0].at[spot], s, r, 3)
        axis = axes[stage - 1]
        away = {a: self.bits[a] for a in axes[:stage - 1]}
        away[axis] = 1 - self.bits[axis]
        dst = bufs[stage].at[(slice(None),) * (3 - stage) + (pl.ds(*rows), slice(None))]
        return self.remote(own.at[view(away, rows)], dst, s, r, axis)

    def rs_step(self, flow, stage):
        own, _, bufs, _, p = flow
        rows, axes = RS_ROWS[p], AXES[p % 3]
        self.rs_copy(flow, stage).wait()
        ref = own.at[view({a: self.bits[a] for a in axes[:stage]}, rows)]
        ref[...] = ref[...] + bufs[stage][(slice(None),) * (3 - stage) + (pl.ds(*rows), slice(None))]
        if stage < 3:
            self.rs_copy(flow, stage + 1).start()

    def ag_copy(self, gat, sems, kind, p, slot):
        rows, axes, bits = AG_ROWS[p], AXES[p % 3], self.bits
        if slot == 0:
            at, axis = {a: bits[a] for a in range(3)}, 3
        elif slot <= 3:
            at, axis = {a: bits[a] for a in axes[slot - 1:]}, axes[slot - 1]
        else:
            at, axis = {a: bits[a] for a in axes[slot - 3:]}, 3
            at[axes[slot - 4]] = 1 - bits[axes[slot - 4]]
        spot = gat.at[(kind, self.core) + view(at, rows)]
        return self.remote(spot, spot, sems[0].at[kind, p, slot], sems[1].at[kind, p, slot], axis)

    def ag_begin(self, *flow):
        self.ag_copy(*flow, 1).start()
        self.ag_copy(*flow, 0).start()

    def ag_step(self, *flow, stage):
        self.ag_copy(*flow, stage).wait()
        if stage < 3:
            self.ag_copy(*flow, stage + 1).start()
        self.ag_copy(*flow, 3 + stage).start()

    def ag_end(self, *flow):
        for slot in (0, 4, 5, 6):
            self.ag_copy(*flow, slot).wait()


def stages():
    return [pltpu.VMEM(CUBE[k:], F32) if k else pltpu.VMEM(CUBE, F32) for k in range(4)]


def kernel_c(tile, tiles, dh_ref, dz_ref, a0_ref, w1_ref, q_ref, rx_hbm,
             g1_ref, sum_ref, ry_hbm,
             r3, rt, blk, own, xa0, xa1, xa2, xa3, xb0, xb1, xb2, xb3, lsem, as_, ar, bs, br):
    i = pl.program_id(0)
    c = Comm()
    bufs = ((xa0, xa1, xa2, xa3), (xb0, xb1, xb2, xb3))
    sems = ((as_, ar), (bs, br))
    flows = [(own.at[k], rx_hbm.at[k, 1 - c.core], bufs[k], sems[k], p) for k in range(2) for p in range(3)]

    def mine():
        return pltpu.make_async_copy(rx_hbm.at[:, c.core], own, lsem.at[0])

    @pl.when(i == 0)
    def _():
        c.greet()
        mine().start()
        r3[...] = jnp.zeros_like(r3)
        c.met()
        for flow in flows:
            c.rs_copy(flow, 0).start()

    @pl.when(i == 2)
    def _():
        mine().wait()

    for at, stage in ((2, 0), (5, 1), (7, 2)):
        @pl.when(i == at)
        def _():
            for flow in flows:
                c.rs_step(flow, stage)

    half = 512
    for n in range(0, D, half):
        g1_ref[:, n:n + half] = (dh_ref[:, n:n + half].astype(F32) + dot_nn(dz_ref[...], w1_ref[:, n:n + half])).astype(BF16)
    v0 = dot_tt(q_ref[...], g1_ref[...]).astype(BF16)
    for s, w in spans_of(512):
        r3[:, s:s + w] += dot_nn(v0, a0_ref[:, s:s + w])

    @pl.when(i == tiles - 1)
    def _():
        leave(r3, rt)
        for d in range(DEV):
            blk[(d % 2) * 8 + d // 2] = rt[SHARD * d:SHARD * d + PAD, :]
        out = pltpu.make_async_copy(blk, ry_hbm, lsem.at[0])
        out.start()
        for flow in flows:
            c.rs_step(flow, 3)
        for k in range(2):
            sum_ref[k] = own[k, c.bits[0], c.bits[1], c.bits[2]]
        out.wait()


def call_c(dh, dz, a0, w1, q, rx):
    rows, tile = dh.shape[0], 512
    tiles = rows // tile
    dma = pltpu.SemaphoreType.DMA
    return pl.pallas_call(
        functools.partial(kernel_c, tile, tiles),
        grid=(tiles,),
        in_specs=[
            pl.BlockSpec((tile, D), lambda i: (i, 0)),
            pl.BlockSpec((tile, FF), lambda i: (i, 0)),
            pl.BlockSpec((tile, FF), lambda i: (i, 0)),
            pl.BlockSpec((None, FF, D), lambda i: (1, 0, 0), pipeline_mode=ONCE),
            pl.BlockSpec((None, D, RANK), lambda i: (0, 0, 0), pipeline_mode=ONCE),
            ANY,
        ],
        out_specs=[
            pl.BlockSpec((tile, D), lambda i: (i, 0)),
            pl.BlockSpec((2, PAD, RANK), lambda i: (0, 0, 0), pipeline_mode=ONCE),
            ANY,
        ],
        out_shape=[
            jax.ShapeDtypeStruct((rows, D), BF16),
            jax.ShapeDtypeStruct((2, PAD, RANK), F32),
            jax.ShapeDtypeStruct((DEV, PAD, RANK), F32),
        ],
        scratch_shapes=[
            pltpu.VMEM((RANK, FFP), F32), pltpu.VMEM((FFP, RANK), F32), pltpu.VMEM((DEV, PAD, RANK), F32),
            pltpu.VMEM((2,) + CUBE, F32), *stages(), *stages(),
            dma((1,)), dma((3, 4)), dma((3, 4)), dma((3, 4)), dma((3, 4)),
        ],
        compiler_params=pltpu.CompilerParams(
            dimension_semantics=("arbitrary",), collective_id=1, has_side_effects=True, vmem_limit_bytes=60000000),
        cost_estimate=pl.CostEstimate(flops=31 * 10**9, bytes_accessed=70 * 10**6, transcendentals=0),
        name="pass_c",
    )(dh, dz, a0, w1, q, rx)


def kernel_d(tile, tiles, width, chunks,
             slope_ref, w2_ref, sum_ref, mu, vu, md, vd, g1_hbm, u0_hbm, rx_hbm,
             mu_o, vu_o, md_o, vd_o, n_hbm,
             g1, u0, das, dz, acc_s, racc, rt, own_x, own_y,
             x0, x1, x2, x3, y0, y1, y2, y3, gat, tmp, nb,
             lsem, rx_s, rx_r, ry_s, ry_r, ag_s, ag_r, nsem):
    j = pl.program_id(0)
    slab = 16
    c = Comm()
    bits, core = c.bits, c.core
    ag_sems = (ag_s, ag_r)
    flows_x = [(own_x, rx_hbm.at[1 - core], (x0, x1, x2, x3), (rx_s, rx_r), p) for p in range(3)]
    flows_y = [(own_y.at[core], own_y.at[1 - core], (y0, y1, y2, y3), (ry_s, ry_r), p) for p in SIXTHS]

    def rs(flows, stage):
        for flow in flows:
            c.rs_step(flow, stage)

    def ag(kinds, stage):
        for kind in kinds:
            for p in SIXTHS if kind == 0 else THIRDS:
                if stage == 0:
                    c.ag_begin(gat, ag_sems, kind, p)
                elif stage < 4:
                    c.ag_step(gat, ag_sems, kind, p, stage=stage)
                else:
                    c.ag_end(gat, ag_sems, kind, p)

    def adam(kind, grad):
        m_i, v_i, m_o, v_o = (mu, vu, mu_o, vu_o) if kind < 2 else (md, vd, md_o, vd_o)
        l = kind % 2
        new_mom, new_var, n = adam_shard(m_i[:, l, :], v_i[:, l, :], grad)
        m_o[:, l, :] = new_mom
        v_o[:, l, :] = new_var
        full = jnp.concatenate([n, jnp.zeros((PAD - SHARD, RANK), F32)], axis=0)
        gat[(kind, core, bits[0], bits[1], bits[2])] = full.astype(BF16)

    def n_copy(kind):
        return pltpu.make_async_copy(nb.at[kind % 2], n_hbm.at[kind], nsem.at[kind])

    def gather_rows(kind):
        for d in range(DEV):
            block = gat[kind, d % 2, d // 8, d // 4 % 2, d // 2 % 2]
            tmp[SHARD * d:SHARD * (d + 1), :] = block.astype(F32)[:SHARD]
        nb[kind % 2] = tmp[...].astype(BF16)
        n_copy(kind).start()

    def local(k):
        src, dst = ((g1_hbm, g1), (u0_hbm, u0), (rx_hbm.at[core], own_x))[k]
        return pltpu.make_async_copy(src, dst, lsem.at[k])

    def begin():
        c.greet()
        for k in range(3):
            local(k).start()
        adam(1, sum_ref[0, 0:SHARD, :])
        adam(3, sum_ref[1, 0:SHARD, :])
        c.met()
        ag((1, 3), 0)
        for flow in flows_x:
            c.rs_copy(flow, 0).start()
        for k in range(3):
            local(k).wait()

    def step_one():
        rs(flows_x, 0)
        ag((1, 3), 1)

    def finish_x():
        rs(flows_x, 3)
        adam(2, own_x[bits[0], bits[1], bits[2], 0:SHARD, :])
        ag((2,), 0)

    events = {0: begin, 1: step_one, 2: lambda: ag((1, 3), 2), 3: lambda: rs(flows_x, 1), 4: lambda: ag((1, 3), 3),
              5: lambda: rs(flows_x, 2), 7: finish_x, 8: lambda: ag((2,), 1), 9: lambda: ag((2,), 2), 10: lambda: ag((2,), 3)}
    for at, event in events.items():
        pl.when(j == at)(event)

    now = lax.rem(j, 2)

    def turn(step):
        rt[pl.ds(pl.multiple_of(step * width, width), width), :] = racc[lax.rem(step, 2)].T

    def act(t):
        k = t % 2
        for r in range(0, tile, slab):
            slope = slope_ref[t * tile + r:t * tile + r + slab, :]
            dz[k, r:r + slab, :] = (slope * das[k, r:r + slab, :]).astype(BF16)

    def acc(t):
        part = dot_nn(u0[:, t * tile:(t + 1) * tile], dz[t % 2])
        if t == tiles - 1:
            racc[now] = acc_s[...] + part
        else:
            acc_s[...] = part if t == 0 else acc_s[...] + part

    turn(lax.rem(j + chunks - 1, chunks))
    for t in range(tiles + 2):
        if t < tiles:
            das[t % 2] = dot_nt(g1[t * tile:(t + 1) * tile, :], w2_ref[...])
        if 1 <= t <= tiles:
            act(t - 1)
        if t >= 2:
            acc(t - 2)

    @pl.when(j == chunks - 1)
    def _():
        turn(j)
        for d in range(DEV):
            own_y[d % 2, d // 8, d // 4 % 2, d // 2 % 2] = rt[SHARD * d:SHARD * d + PAD, :]
        for flow in flows_y:
            c.rs_copy(flow, 0).start()
        ag((1, 3), 4)
        gather_rows(1)
        rs(flows_y, 0)
        ag((2,), 4)
        gather_rows(2)
        rs(flows_y, 1)
        n_copy(1).wait()
        gather_rows(3)
        rs(flows_y, 2)
        rs(flows_y, 3)
        adam(0, own_y[core, bits[0], bits[1], bits[2], 0:SHARD, :])
        for stage in range(5):
            ag((0,), stage)
        n_copy(2).wait()
        gather_rows(0)
        n_copy(3).wait()
        n_copy(0).wait()


def call_d(z0, g1, u0, w2, sums, rx, mu, vu, md, vd):
    rows, tile, width = z0.shape[0], 512, 256
    chunks = FFP // width
    mom = jax.ShapeDtypeStruct((SHARD, 2, RANK), F32)
    momspec = pl.BlockSpec((SHARD, 2, RANK), lambda j: (0, 0, 0), pipeline_mode=ONCE)
    dma = pltpu.SemaphoreType.DMA
    return pl.pallas_call(
        functools.partial(kernel_d, tile, rows // tile, width, chunks),
        grid=(chunks,),
        in_specs=[
            pl.BlockSpec((rows, width), lambda j: (0, j)),
            pl.BlockSpec((None, width, D), lambda j: (0, j, 0)),
            pl.BlockSpec((2, PAD, RANK), lambda j: (0, 0, 0), pipeline_mode=ONCE),
            momspec, momspec, momspec, momspec, ANY, ANY, ANY,
        ],
        out_specs=[momspec] * 4 + [ANY],
        out_shape=[mom] * 4 + [jax.ShapeDtypeStruct((4, FF, RANK), BF16)],
        scratch_shapes=[
            pltpu.VMEM((rows, D), BF16), pltpu.VMEM((RANK, rows), BF16),
            pltpu.VMEM((2, tile, width), F32), pltpu.VMEM((2, tile, width), BF16),
            pltpu.VMEM((RANK, width), F32), pltpu.VMEM((2, RANK, width), F32), pltpu.VMEM((FFP, RANK), F32),
            pltpu.VMEM(CUBE, F32), pltpu.VMEM((2,) + CUBE, F32), *stages(), *stages(),
            pltpu.VMEM((4, 2) + CUBE, BF16), pltpu.VMEM((FF, RANK), F32), pltpu.VMEM((2, FF, RANK), BF16),
            dma((3,)), dma((3, 4)), dma((3, 4)), dma((9, 4)), dma((9, 4)), dma((4, 9, 7)), dma((4, 9, 7)), dma((4,)),
        ],
        compiler_params=pltpu.CompilerParams(
            dimension_semantics=("arbitrary",), collective_id=0, has_side_effects=True, vmem_limit_bytes=67000000),
        cost_estimate=pl.CostEstimate(flops=30 * 10**9, bytes_accessed=70 * 10**6, transcendentals=0),
        name="pass_d",
    )(z0, w2, sums, mu, vu, md, vd, g1, u0, rx)


def kernel_w(count, part, wu_hbm, wd_hbm, n_hbm, p_ref, q_ref, nu_hbm, nd_hbm, buf, n, isem, nsem, osem):
    per = FF // part

    def load(k):
        src, at = (wu_hbm, k) if k < 2 * per else (wd_hbm, k - 2 * per)
        return pltpu.make_async_copy(src.at[at], buf.at[k], isem.at[k])

    def names(kind):
        return pltpu.make_async_copy(n_hbm.at[pl.ds(kind * per, per)], n.at[pl.ds(kind * per, per)], nsem.at[kind])

    ahead = AHEAD
    for k in range(count):
        if k % per == 0:
            names(k // per).start()
        if k < ahead:
            load(k).start()
    for kind in range(4):
        proj, dst, base = (p_ref, nu_hbm, 0) if kind < 2 else (q_ref, nd_hbm, 2 * per)
        names(kind).wait()

        def body(t, carry):
            k = kind * per + t
            pltpu.make_async_copy(wu_hbm.at[0], buf.at[k], isem.at[k]).wait()
            more = k + ahead

            @pl.when(more < 2 * per)
            def _():
                pltpu.make_async_copy(wu_hbm.at[more], buf.at[more], isem.at[more]).start()

            @pl.when(jnp.logical_and(more >= 2 * per, more < count))
            def _():
                pltpu.make_async_copy(wd_hbm.at[more - 2 * per], buf.at[more], isem.at[more]).start()

            for s in range(0, D, 256):
                delta = dot_nt(n[k], proj[kind % 2, s:s + 256, :])
                buf[k, :, s:s + 256] = (buf[k, :, s:s + 256].astype(F32) - (LEARN_RATE * ALPHA_SCALE) * delta).astype(BF16)
            pltpu.make_async_copy(buf.at[k], dst.at[k - base], osem.at[k]).start()
            return carry

        lax.fori_loop(0, per, body, 0)
    for k in range(count):
        dst, at = (nu_hbm, k) if k < 2 * per else (nd_hbm, k - 2 * per)
        pltpu.make_async_copy(buf.at[k], dst.at[at], osem.at[k]).wait()


def call_w(wu, wd, n, p, q):
    part = 456
    per = FF // part
    count = 4 * per
    whole = pl.BlockSpec(memory_space=pltpu.VMEM)
    out = jax.ShapeDtypeStruct((2 * per, part, D), BF16)
    dma = pltpu.SemaphoreType.DMA
    nu, nd = pl.pallas_call(
        functools.partial(kernel_w, count, part),
        in_specs=[ANY, ANY, ANY, whole, whole],
        out_specs=[ANY, ANY],
        out_shape=[out, out],
        scratch_shapes=[pltpu.VMEM((count, part, D), BF16), pltpu.VMEM((count, part, RANK), BF16), dma((count,)), dma((4,)), dma((count,))],
        compiler_params=pltpu.CompilerParams(vmem_limit_bytes=60000000),
        cost_estimate=pl.CostEstimate(flops=6 * 10**9, bytes_accessed=50 * 10**6, transcendentals=0),
        name="pass_w",
    )(wu.reshape(2 * per, part, D), wd.reshape(2 * per, part, D), n.reshape(count, part, RANK), p, q)
    return nu.reshape(2, FF, D), nd.reshape(2, FF, D)


def solution(mesh):
    def local_step(x_loc, dh_loc, w_up, w_down, proj_up, proj_down, mom_up, var_up, mom_down, var_down):
        w_up_t = jnp.swapaxes(w_up, 1, 2)
        z0, a0, dz1, u0, rx = call_a(x_loc, dh_loc, proj_up, proj_down, w_up_t, w_down)
        g1, sums, ry = call_c(dh_loc, dz1, a0, w_up_t, proj_down, rx.reshape((2, 2) + CUBE))
        up, down = (2, 0, 1), (1, 0, 2)
        mu, vu, md, vd, dirs = call_d(
            z0, g1, u0, w_down, sums, ry.reshape((2,) + CUBE), jnp.transpose(mom_up, up), jnp.transpose(var_up, up),
            jnp.transpose(mom_down, down), jnp.transpose(var_down, down))
        new_mom_up, new_var_up = jnp.transpose(mu, (1, 2, 0)), jnp.transpose(vu, (1, 2, 0))
        new_mom_down, new_var_down = jnp.transpose(md, (1, 0, 2)), jnp.transpose(vd, (1, 0, 2))
        new_up, new_w_down = call_w(w_up_t, w_down, dirs, proj_up, proj_down)
        return jnp.swapaxes(new_up, 1, 2), new_w_down, new_mom_up, new_var_up, new_mom_down, new_var_down

    tok_spec = P('data', None)
    up_spec = P(None, None, 'data')
    down_spec = P(None, 'data', None)
    return jax.shard_map(
        local_step,
        mesh=mesh,
        in_specs=(tok_spec, tok_spec, P(), P(), P(), P(), up_spec, up_spec, down_spec, down_spec),
        out_specs=(P(), P(), up_spec, up_spec, down_spec, down_spec),
        check_vma=False,
    )
```

```python
import functools

import jax
import jax.numpy as jnp
from jax import lax
from jax.experimental import pallas as pl
from jax.experimental.pallas import tpu as pltpu
from jax.sharding import PartitionSpec as P

BETA_ONE = 0.9
BETA_TWO = 0.999
EPSILON = 1e-8
STEP = 4
LEARN_RATE = 0.02
ALPHA_SCALE = 0.25

C0 = 0.7978845608028654
C1 = C0 * 0.044715
D = 1024
FF = 2736
RANK = 256
DEV = 16
SHARD = FF // DEV
PAD = 176
FFP = DEV * PAD
F32 = jnp.float32
BF16 = jnp.bfloat16


def spans_of(width):
    return [(s, min(width, FF - s)) for s in range(0, FF, width)]


def pieces(span, width=256):
    s, w = span
    return [(t, min(width, s + w - t)) for t in range(s, s + w, width)]


def dot_nn(a, b):
    return lax.dot_general(a, b, (((1,), (0,)), ((), ())), preferred_element_type=F32)


def dot_nt(a, b):
    return lax.dot_general(a, b, (((1,), (1,)), ((), ())), preferred_element_type=F32)


def dot_tt(a, b):
    return lax.dot_general(a, b, (((0,), (1,)), ((), ())), preferred_element_type=F32)


def gelu_both(z):
    z2 = z * z
    t = jnp.tanh(z * (C0 + C1 * z2))
    c = 0.5 * t + 0.5
    a = z * c
    slope = c + (a - a * c) * (2.0 * C0 + 6.0 * C1 * z2)
    return a, slope


ANY = pl.BlockSpec(memory_space=pl.ANY)
ONCE = pl.Buffered(1)


def kernel_a(tile, tiles, x_ref, dh_ref, p_ref, q_ref, w1_hbm, w2_hbm,
             slope_hbm, g1_hbm, u0_ref, r_hbm,
             w1a, w2a, w1b, w2b, slope, a0, h1, dz1, zs, das, ac, u1, v1, r1, r2, r3, blk, sem, zsem):
    i = pl.program_id(0)
    width, slab = 512, 16
    spans = spans_of(width)
    loads = [
        pltpu.make_async_copy(w1_hbm.at[0], w1a, sem.at[0]),
        pltpu.make_async_copy(w2_hbm.at[0], w2a, sem.at[1]),
        pltpu.make_async_copy(w1_hbm.at[1], w1b, sem.at[2]),
        pltpu.make_async_copy(w2_hbm.at[1], w2b, sem.at[3]),
    ]

    chunks = FFP // 256

    def out(idx, k):
        rows = pl.ds(pl.multiple_of(idx * tile, tile), tile)
        if k == chunks:
            return pltpu.make_async_copy(h1, g1_hbm.at[rows], zsem.at[k])
        return pltpu.make_async_copy(slope.at[:, k * 256:k * 256 + 256], slope_hbm.at[k, rows], zsem.at[k])

    def outs(idx):
        return [out(idx, k) for k in range(chunks + 1)]

    @pl.when(i == 0)
    def _():
        for cp in loads:
            cp.start()
        r1[...] = jnp.zeros_like(r1)
        r2[...] = jnp.zeros_like(r2)
        r3[...] = jnp.zeros_like(r3)
        for cp in loads:
            cp.wait()

    @pl.when(i > 0)
    def _():
        for cp in outs(i - 1):
            cp.wait()

    x = x_ref[...]
    dh = dh_ref[...]

    def act0(span, k):
        for s, w in pieces(span):
            o = s - span[0]
            for r in range(0, tile, slab):
                a, g = gelu_both(zs[k, r:r + slab, o:o + w])
                a0[r:r + slab, s:s + w] = a.astype(BF16)
                slope[r:r + slab, s:s + w] = g

    n = len(spans)
    for j in range(n + 1):
        if j < n:
            s, w = spans[j]
            zs[j % 2, :, :w] = dot_nt(x, w1a[s:s + w, :])
        else:
            u0_ref[...] = dot_tt(p_ref[0], x).astype(BF16)
            v1[...] = dot_tt(q_ref[1], dh).astype(BF16)
        if j > 0:
            act0(spans[j - 1], (j - 1) % 2)

    for n in range(0, D, width):
        h1[:, n:n + width] = (x_ref[:, n:n + width].astype(F32) + dot_nn(a0[...], w2a[:, n:n + width])).astype(BF16)
    for k in range(chunks):
        out(i, k).start()

    def act1(span, k):
        for s, w in pieces(span):
            o = s - span[0]
            for r in range(0, tile, slab):
                a, g = gelu_both(zs[k, r:r + slab, o:o + w])
                ac[k, r:r + slab, o:o + w] = a.astype(BF16)
                dz1[r:r + slab, s:s + w] = (g * das[k, r:r + slab, o:o + w]).astype(BF16)

    def acc1(span, k):
        s, w = span
        r2[:, s:s + w] += dot_nn(v1[...], ac[k, :, :w])
        r1[:, s:s + w] += dot_nn(u1[...], dz1[:, s:s + w])

    h = h1[...]
    n = len(spans)
    for j in range(n + 2):
        if j < n:
            s, w = spans[j]
            das[j % 2, :, :w] = dot_nt(dh, w2b[s:s + w, :])
            zs[j % 2, :, :w] = dot_nt(h, w1b[s:s + w, :])
        if j == 0:
            u1[...] = dot_tt(p_ref[1], h).astype(BF16)
        if 1 <= j <= n:
            act1(spans[j - 1], (j - 1) % 2)
        if j >= 2:
            acc1(spans[j - 2], (j - 2) % 2)

    for n in range(0, D, width):
        h1[:, n:n + width] = (dh_ref[:, n:n + width].astype(F32) + dot_nn(dz1[...], w1b[:, n:n + width])).astype(BF16)
    v0 = dot_tt(q_ref[0], h1[...]).astype(BF16)
    out(i, chunks).start()
    for s, w in spans:
        r3[:, s:s + w] += dot_nn(v0, a0[:, s:s + w])

    @pl.when(i == tiles - 1)
    def _():
        for cp in outs(i):
            cp.wait()
        for k, acc in enumerate((r1, r2, r3)):
            for t in range(FFP // 256):
                slope[t % 2 * 256:t % 2 * 256 + 256, t // 2 * 256:t // 2 * 256 + 256] = acc[:, t * 256:t * 256 + 256].T
            if k > 0:
                pltpu.make_async_copy(blk, r_hbm.at[k - 1], sem.at[k - 1]).wait()
            for d in range(DEV):
                row, end = SHARD * d, SHARD * d + PAD
                while row < end:
                    t, lo = row // 256, row % 256
                    take = min(end - row, 256 - lo)
                    to = row - SHARD * d
                    blk[(d % 2) * 8 + d // 2, to:to + take, :] = slope[t % 2 * 256 + lo:t % 2 * 256 + lo + take, t // 2 * 256:t // 2 * 256 + 256]
                    row += take
            pltpu.make_async_copy(blk, r_hbm.at[k], sem.at[k]).start()
        pltpu.make_async_copy(blk, r_hbm.at[2], sem.at[2]).wait()


def call_a(x, dh, p, q, w1, w2):
    rows, tile = x.shape[0], 512
    tiles = rows // tile
    whole = pl.BlockSpec((2, D, RANK), lambda i: (0, 0, 0), pipeline_mode=ONCE)
    rowspec = pl.BlockSpec((tile, D), lambda i: (i, 0))
    return pl.pallas_call(
        functools.partial(kernel_a, tile, tiles),
        grid=(tiles,),
        in_specs=[rowspec, rowspec, whole, whole, ANY, ANY],
        out_specs=[ANY, ANY, pl.BlockSpec((RANK, tile), lambda i: (0, i)), ANY],
        out_shape=[
            jax.ShapeDtypeStruct((FFP // 256, rows, 256), F32),
            jax.ShapeDtypeStruct((rows, D), BF16),
            jax.ShapeDtypeStruct((RANK, rows), BF16),
            jax.ShapeDtypeStruct((3, DEV, PAD, RANK), F32),
        ],
        scratch_shapes=[
            pltpu.VMEM((FF, D), BF16), pltpu.VMEM((FF, D), BF16),
            pltpu.VMEM((FF, D), BF16), pltpu.VMEM((FF, D), BF16),
            pltpu.VMEM((tile, FFP), F32), pltpu.VMEM((tile, FF), BF16), pltpu.VMEM((tile, D), BF16), pltpu.VMEM((tile, FF), BF16),
            pltpu.VMEM((2, tile, 512), F32), pltpu.VMEM((2, tile, 512), F32), pltpu.VMEM((2, tile, 512), BF16),
            pltpu.VMEM((RANK, tile), BF16), pltpu.VMEM((RANK, tile), BF16),
            pltpu.VMEM((RANK, FFP), F32), pltpu.VMEM((RANK, FFP), F32), pltpu.VMEM((RANK, FFP), F32),
            pltpu.VMEM((DEV, PAD, RANK), F32),
            pltpu.SemaphoreType.DMA((4,)), pltpu.SemaphoreType.DMA((FFP // 256 + 1,)),
        ],
        compiler_params=pltpu.CompilerParams(
            dimension_semantics=("arbitrary",), vmem_limit_bytes=67000000),
        cost_estimate=pl.CostEstimate(flops=110 * 10**9, bytes_accessed=140 * 10**6, transcendentals=0),
        name="pass_a",
    )(x, dh, p, q, w1, w2)


def adam_shard(moment, variance, grad_red):
    new_mom = BETA_ONE * moment + (1.0 - BETA_ONE) * grad_red
    new_var = BETA_TWO * variance + (1.0 - BETA_TWO) * grad_red * grad_red
    bias_one = 1.0 - BETA_ONE ** STEP
    bias_two = 1.0 - BETA_TWO ** STEP
    direction = (new_mom / bias_one) / (jnp.sqrt(new_var / bias_two) + EPSILON)
    return new_mom, new_var, direction


AHEAD = 10
AXES = ((2, 1, 0), (1, 0, 2), (0, 2, 1))
RS_ROWS = ((0, 56), (56, 56), (112, 64), (0, 24), (56, 24), (112, 32), (24, 32), (80, 32), (144, 32))
AG_ROWS = ((0, 48), (48, 64), (112, 64), (0, 16), (48, 32), (112, 32), (16, 32), (80, 32), (144, 32))
THIRDS, SIXTHS = range(3), range(3, 9)
MESH = pl.DeviceIdType.MESH
CUBE = (2, 2, 2, PAD, RANK)


def view(fixed, rows):
    return tuple(fixed.get(a, slice(None)) for a in range(3)) + (pl.ds(*rows), slice(None))


class Comm:
    def __init__(self):
        me = lax.axis_index('data')
        self.bits = [lax.rem(me // (8 >> a), 2) for a in range(4)]
        self.peer = [me + (1 - 2 * self.bits[a]) * (8 >> a) for a in range(4)]
        self.core = self.bits[3]

    def greet(self):
        barrier = pltpu.get_barrier_semaphore()
        for a in range(4):
            pl.semaphore_signal(barrier, inc=1, device_id=(self.peer[a],), device_id_type=MESH)

    def met(self):
        pl.semaphore_wait(pltpu.get_barrier_semaphore(), 4)

    def remote(self, src, dst, s, r, axis):
        return pltpu.make_async_remote_copy(src_ref=src, dst_ref=dst, send_sem=s, recv_sem=r,
                                            device_id=(self.peer[axis],), device_id_type=MESH)

    def rs_copy(self, flow, stage):
        own, other, bufs, sems, p = flow
        rows, axes = RS_ROWS[p], AXES[p % 3]
        s, r = (sem.at[p, stage] for sem in sems)
        if stage == 0:
            spot = view({}, rows)
            return self.remote(other.at[spot], bufs[0].at[spot], s, r, 3)
        axis = axes[stage - 1]
        away = {a: self.bits[a] for a in axes[:stage - 1]}
        away[axis] = 1 - self.bits[axis]
        dst = bufs[stage].at[(slice(None),) * (3 - stage) + (pl.ds(*rows), slice(None))]
        return self.remote(own.at[view(away, rows)], dst, s, r, axis)

    def rs_step(self, flow, stage):
        own, _, bufs, _, p = flow
        rows, axes = RS_ROWS[p], AXES[p % 3]
        self.rs_copy(flow, stage).wait()
        ref = own.at[view({a: self.bits[a] for a in axes[:stage]}, rows)]
        ref[...] = ref[...] + bufs[stage][(slice(None),) * (3 - stage) + (pl.ds(*rows), slice(None))]
        if stage < 3:
            self.rs_copy(flow, stage + 1).start()

    def ag_copy(self, gat, sems, kind, p, slot):
        rows, axes, bits = AG_ROWS[p], AXES[p % 3], self.bits
        if slot == 0:
            at, axis = {a: bits[a] for a in range(3)}, 3
        elif slot <= 3:
            at, axis = {a: bits[a] for a in axes[slot - 1:]}, axes[slot - 1]
        else:
            at, axis = {a: bits[a] for a in axes[slot - 3:]}, 3
            at[axes[slot - 4]] = 1 - bits[axes[slot - 4]]
        spot = gat.at[(kind, self.core) + view(at, rows)]
        return self.remote(spot, spot, sems[0].at[kind, p, slot], sems[1].at[kind, p, slot], axis)

    def ag_begin(self, *flow):
        self.ag_copy(*flow, 1).start()
        self.ag_copy(*flow, 0).start()

    def ag_step(self, *flow, stage):
        self.ag_copy(*flow, stage).wait()
        if stage < 3:
            self.ag_copy(*flow, stage + 1).start()
        self.ag_copy(*flow, 3 + stage).start()

    def ag_end(self, *flow):
        for slot in (0, 4, 5, 6):
            self.ag_copy(*flow, slot).wait()


def stages():
    return [pltpu.VMEM(CUBE[k:], F32) if k else pltpu.VMEM(CUBE, F32) for k in range(4)]


def kernel_d(tile, tiles, width, chunks,
             slope_ref, w2_ref, mu, vu, md, vd, g1_hbm, u0_hbm, rx_hbm,
             mu_o, vu_o, md_o, vd_o, n_hbm,
             g1, u0, das, dz, acc_s, racc, rt, own_x, own_y,
             xa0, xa1, xa2, xa3, xb0, xb1, xb2, xb3, xc0, xc1, xc2, xc3, y0, y1, y2, y3, gat, tmp, nb,
             lsem, xa_s, xa_r, xb_s, xb_r, xc_s, xc_r, ry_s, ry_r, ag_s, ag_r, nsem):
    j = pl.program_id(0)
    slab = 16
    c = Comm()
    bits, core = c.bits, c.core
    ag_sems = (ag_s, ag_r)
    bufs = ((xa0, xa1, xa2, xa3), (xb0, xb1, xb2, xb3), (xc0, xc1, xc2, xc3))
    sems = ((xa_s, xa_r), (xb_s, xb_r), (xc_s, xc_r))
    kinds = (1, 3, 2)
    flows_x = [[(own_x.at[k], rx_hbm.at[k, 1 - core], bufs[k], sems[k], p) for p in THIRDS] for k in range(3)]
    flows_y = [(own_y.at[core], own_y.at[1 - core], (y0, y1, y2, y3), (ry_s, ry_r), p) for p in SIXTHS]

    def rs(flows, stage):
        for flow in flows:
            c.rs_step(flow, stage)

    def ag(kinds, stage):
        for kind in kinds:
            for p in SIXTHS if kind == 0 else THIRDS:
                if stage == 0:
                    c.ag_begin(gat, ag_sems, kind, p)
                elif stage < 4:
                    c.ag_step(gat, ag_sems, kind, p, stage=stage)
                else:
                    c.ag_end(gat, ag_sems, kind, p)

    def adam(kind, grad):
        m_i, v_i, m_o, v_o = (mu, vu, mu_o, vu_o) if kind < 2 else (md, vd, md_o, vd_o)
        l = kind % 2
        new_mom, new_var, n = adam_shard(m_i[:, l, :], v_i[:, l, :], grad)
        m_o[:, l, :] = new_mom
        v_o[:, l, :] = new_var
        full = jnp.concatenate([n, jnp.zeros((PAD - SHARD, RANK), F32)], axis=0)
        gat[(kind, core, bits[0], bits[1], bits[2])] = full.astype(BF16)

    def n_copy(kind):
        return pltpu.make_async_copy(nb.at[kind % 2], n_hbm.at[kind], nsem.at[kind])

    def gather_rows(kind):
        for d in range(DEV):
            block = gat[kind, d % 2, d // 8, d // 4 % 2, d // 2 % 2]
            tmp[SHARD * d:SHARD * (d + 1), :] = block.astype(F32)[:SHARD]
        nb[kind % 2] = tmp[...].astype(BF16)
        n_copy(kind).start()

    def local(k):
        src, dst = ((g1_hbm, g1), (u0_hbm, u0), (rx_hbm.at[:, core], own_x))[k]
        return pltpu.make_async_copy(src, dst, lsem.at[k])

    def begin():
        c.greet()
        for k in range(3):
            local(k).start()
        c.met()
        for k in range(3):
            for flow in flows_x[k]:
                c.rs_copy(flow, 0).start()
        for k in range(3):
            local(k).wait()

    def finish_x():
        for k in range(3):
            rs(flows_x[k], 3)
            adam(kinds[k], own_x[k, bits[0], bits[1], bits[2], 0:SHARD, :])
            ag((kinds[k],), 0)
        add_y(0)

    def all_zero():
        for k in range(3):
            rs(flows_x[k], 0)

    def cross_y(z):
        return c.remote(own_y.at[1 - core, z], y0.at[z], ry_s.at[z, 0], ry_r.at[z, 0], 3)

    def early_y(z):
        for d in range(8 * z, 8 * z + 8):
            own_y[d % 2, z, d // 4 % 2, d // 2 % 2] = rt[SHARD * d:SHARD * d + PAD, :]
        cross_y(z).start()

    def add_y(z):
        cross_y(z).wait()
        own_y[core, z] = own_y[core, z] + y0[z]

    events = {0: begin, 1: all_zero, 3: lambda: rs(flows_x[0], 1), 4: lambda: rs(flows_x[1], 1), 5: lambda: rs(flows_x[2], 1),
              6: lambda: rs(flows_x[0], 2), 7: lambda: (rs(flows_x[1], 2), rs(flows_x[2], 2), early_y(0)),
              8: finish_x, 9: lambda: ag(kinds, 1), 10: lambda: ag(kinds, 2)}
    for at, event in events.items():
        pl.when(j == at)(lambda event=event: [event(), None][1])

    now = lax.rem(j, 2)

    def turn(step):
        rt[pl.ds(pl.multiple_of(step * width, width), width), :] = racc[lax.rem(step, 2)].T

    def act(t):
        k = t % 2
        for r in range(0, tile, slab):
            slope = slope_ref[t * tile + r:t * tile + r + slab, :]
            dz[k, r:r + slab, :] = (slope * das[k, r:r + slab, :]).astype(BF16)

    def acc(t):
        part = dot_nn(u0[:, t * tile:(t + 1) * tile], dz[t % 2])
        if t == tiles - 1:
            racc[now] = acc_s[...] + part
        else:
            acc_s[...] = part if t == 0 else acc_s[...] + part

    turn(lax.rem(j + chunks - 1, chunks))
    for t in range(tiles + 2):
        if t < tiles:
            das[t % 2] = dot_nt(g1[t * tile:(t + 1) * tile, :], w2_ref[...])
        if 1 <= t <= tiles:
            act(t - 1)
        if t >= 2:
            acc(t - 2)

    @pl.when(j == chunks - 1)
    def _():
        turn(j)
        early_y(1)
        add_y(1)
        for flow in flows_y:
            c.rs_copy(flow, 1).start()
        ag(kinds, 3)
        rs(flows_y, 1)
        ag((1,), 4)
        gather_rows(1)
        rs(flows_y, 2)
        ag((2,), 4)
        gather_rows(2)
        ag((3,), 4)
        n_copy(1).wait()
        gather_rows(3)
        rs(flows_y, 3)
        adam(0, own_y[core, bits[0], bits[1], bits[2], 0:SHARD, :])
        for stage in range(5):
            ag((0,), stage)
        n_copy(2).wait()
        gather_rows(0)
        n_copy(3).wait()
        n_copy(0).wait()


def call_d(slope, g1, u0, w2, rx, mu, vu, md, vd):
    rows, tile, width = g1.shape[0], 512, 256
    chunks = FFP // width
    mom = jax.ShapeDtypeStruct((SHARD, 2, RANK), F32)
    momspec = pl.BlockSpec((SHARD, 2, RANK), lambda j: (0, 0, 0), pipeline_mode=ONCE)
    dma = pltpu.SemaphoreType.DMA
    return pl.pallas_call(
        functools.partial(kernel_d, tile, rows // tile, width, chunks),
        grid=(chunks,),
        in_specs=[
            pl.BlockSpec((None, rows, width), lambda j: (j, 0, 0)),
            pl.BlockSpec((None, width, D), lambda j: (0, j, 0)),
            momspec, momspec, momspec, momspec, ANY, ANY, ANY,
        ],
        out_specs=[momspec] * 4 + [ANY],
        out_shape=[mom] * 4 + [jax.ShapeDtypeStruct((4, FF, RANK), BF16)],
        scratch_shapes=[
            pltpu.VMEM((rows, D), BF16), pltpu.VMEM((RANK, rows), BF16),
            pltpu.VMEM((2, tile, width), F32), pltpu.VMEM((2, tile, width), BF16),
            pltpu.VMEM((RANK, width), F32), pltpu.VMEM((2, RANK, width), F32), pltpu.VMEM((FFP, RANK), F32),
            pltpu.VMEM((3,) + CUBE, F32), pltpu.VMEM((2,) + CUBE, F32), *stages(), *stages(), *stages(), *stages(),
            pltpu.VMEM((4, 2) + CUBE, BF16), pltpu.VMEM((FF, RANK), F32), pltpu.VMEM((2, FF, RANK), BF16),
            dma((3,)), *[dma((3, 4))] * 6, dma((9, 4)), dma((9, 4)), dma((4, 9, 7)), dma((4, 9, 7)), dma((4,)),
        ],
        compiler_params=pltpu.CompilerParams(
            dimension_semantics=("arbitrary",), collective_id=0, has_side_effects=True, vmem_limit_bytes=67000000),
        cost_estimate=pl.CostEstimate(flops=30 * 10**9, bytes_accessed=70 * 10**6, transcendentals=0),
        name="pass_d",
    )(slope, w2, mu, vu, md, vd, g1, u0, rx)


def kernel_w(count, part, wu_hbm, wd_hbm, n_hbm, p_ref, q_ref, nu_hbm, nd_hbm, buf, n, isem, nsem, osem):
    per = FF // part

    def load(k):
        src, at = (wu_hbm, k) if k < 2 * per else (wd_hbm, k - 2 * per)
        return pltpu.make_async_copy(src.at[at], buf.at[k], isem.at[k])

    def names(kind):
        return pltpu.make_async_copy(n_hbm.at[pl.ds(kind * per, per)], n.at[pl.ds(kind * per, per)], nsem.at[kind])

    ahead = AHEAD
    for k in range(count):
        if k % per == 0:
            names(k // per).start()
        if k < ahead:
            load(k).start()
    for kind in range(4):
        proj, dst, base = (p_ref, nu_hbm, 0) if kind < 2 else (q_ref, nd_hbm, 2 * per)
        names(kind).wait()

        def body(t, carry):
            k = kind * per + t
            pltpu.make_async_copy(wu_hbm.at[0], buf.at[k], isem.at[k]).wait()
            more = k + ahead

            @pl.when(more < 2 * per)
            def _():
                pltpu.make_async_copy(wu_hbm.at[more], buf.at[more], isem.at[more]).start()

            @pl.when(jnp.logical_and(more >= 2 * per, more < count))
            def _():
                pltpu.make_async_copy(wd_hbm.at[more - 2 * per], buf.at[more], isem.at[more]).start()

            for s in range(0, D, 256):
                delta = dot_nt(n[k], proj[kind % 2, s:s + 256, :])
                buf[k, :, s:s + 256] = (buf[k, :, s:s + 256].astype(F32) - (LEARN_RATE * ALPHA_SCALE) * delta).astype(BF16)
            pltpu.make_async_copy(buf.at[k], dst.at[k - base], osem.at[k]).start()
            return carry

        lax.fori_loop(0, per, body, 0)
    for k in range(count):
        dst, at = (nu_hbm, k) if k < 2 * per else (nd_hbm, k - 2 * per)
        pltpu.make_async_copy(buf.at[k], dst.at[at], osem.at[k]).wait()


def call_w(wu, wd, n, p, q):
    part = 456
    per = FF // part
    count = 4 * per
    whole = pl.BlockSpec(memory_space=pltpu.VMEM)
    out = jax.ShapeDtypeStruct((2 * per, part, D), BF16)
    dma = pltpu.SemaphoreType.DMA
    nu, nd = pl.pallas_call(
        functools.partial(kernel_w, count, part),
        in_specs=[ANY, ANY, ANY, whole, whole],
        out_specs=[ANY, ANY],
        out_shape=[out, out],
        scratch_shapes=[pltpu.VMEM((count, part, D), BF16), pltpu.VMEM((count, part, RANK), BF16), dma((count,)), dma((4,)), dma((count,))],
        compiler_params=pltpu.CompilerParams(vmem_limit_bytes=60000000),
        cost_estimate=pl.CostEstimate(flops=6 * 10**9, bytes_accessed=50 * 10**6, transcendentals=0),
        name="pass_w",
    )(wu.reshape(2 * per, part, D), wd.reshape(2 * per, part, D), n.reshape(count, part, RANK), p, q)
    return nu.reshape(2, FF, D), nd.reshape(2, FF, D)


def solution(mesh):
    def local_step(x_loc, dh_loc, w_up, w_down, proj_up, proj_down, mom_up, var_up, mom_down, var_down):
        w_up_t = jnp.swapaxes(w_up, 1, 2)
        slope, g1, u0, rx = call_a(x_loc, dh_loc, proj_up, proj_down, w_up_t, w_down)
        up, down = (2, 0, 1), (1, 0, 2)
        mu, vu, md, vd, dirs = call_d(
            slope, g1, u0, w_down, rx.reshape((3, 2) + CUBE), jnp.transpose(mom_up, up), jnp.transpose(var_up, up),
            jnp.transpose(mom_down, down), jnp.transpose(var_down, down))
        new_mom_up, new_var_up = jnp.transpose(mu, (1, 2, 0)), jnp.transpose(vu, (1, 2, 0))
        new_mom_down, new_var_down = jnp.transpose(md, (1, 0, 2)), jnp.transpose(vd, (1, 0, 2))
        new_up, new_w_down = call_w(w_up_t, w_down, dirs, proj_up, proj_down)
        return jnp.swapaxes(new_up, 1, 2), new_w_down, new_mom_up, new_var_up, new_mom_down, new_var_down

    tok_spec = P('data', None)
    up_spec = P(None, None, 'data')
    down_spec = P(None, 'data', None)
    return jax.shard_map(
        local_step,
        mesh=mesh,
        in_specs=(tok_spec, tok_spec, P(), P(), P(), P(), up_spec, up_spec, down_spec, down_spec),
        out_specs=(P(), P(), up_spec, up_spec, down_spec, down_spec),
        check_vma=False,
    )
```
